256 devices in a mesh: tm: 8 (over x, core), space: 32 (over z, y).
Axes of the slice: x: 4, y: 4, z: 8, core: 2. Of those that a mesh axis runs over, the one named last changes fastest.
Arguments:
- video_in: bfloat16 [32, 32, 16, 3072], P('tm', 'space'), may hold values from -6 to 6
- neighbours: int32 [32, 8], replicated, may hold values from 0 to 32, as said below
- valid_frames: int32 [32], replicated, may hold values from 0 to 32, as said below
- norm1_gain: float32 [192], replicated, may hold values from 0.1 to 1.9
- conv1_weight: bfloat16 [9, 576, 192], replicated, may hold values from -0.078125 to 0.078125
- conv1_bias: float32 [192], replicated, may hold values from -3 to 3
- norm2_gain: float32 [192], replicated, may hold values from 0.1 to 1.9
- conv2_weight: bfloat16 [9, 576, 192], replicated, may hold values from -0.078125 to 0.078125
- conv2_bias: float32 [192], replicated, may hold values from -3 to 3
Outputs:
- block_out: bfloat16 [32, 32, 16, 3072], P('tm', 'space')
The draws below stay inside these ranges and needn't reach their ends.
Inputs may be any that keep to these rules, and one draw needn't show every extreme that they name: `neighbours`: entry k of a tile's row names the tile beside it in direction k of one placement of all tiles on a grid of 4 rows by 8 columns, directions ordered (row, column) = (-1,-1), (-1,0), (-1,1), (0,-1), (0,1), (1,-1), (1,0), (1,1); 32 where that place lies outside the grid. `valid_frames`: frames from this number on are padding in that tile's track.
All inputs are finite; a program needn't handle non-finite values.
Results may differ from the reference program's by a relative error of at most 0.0037.
Values may be sent and summed in bfloat16 or wider, within the bound.
A program may use at most 64 MiB of HBM per device.

```python
import jax
import jax.numpy as jnp
from jax import lax

C = 192
TS = 16
GRID_W = 8
TILES = 32
GH = 4
F = 32


def tile_layout(key):
    row_key = jax.random.fold_in(key, 101)
    col_key = jax.random.fold_in(key, 102)
    row_order = jax.random.permutation(row_key, GH)

    def shuffled(subkey):
        return jax.random.permutation(subkey, GRID_W)
    col_order = jax.vmap(shuffled)(jax.random.split(col_key, GH))
    grid_row = jnp.repeat(row_order, GRID_W).astype(jnp.int32)
    grid_col = col_order.reshape(-1).astype(jnp.int32)
    return (grid_row, grid_col)


def draw_neighbours(key, part):
    grid_row, grid_col = tile_layout(key)
    placed = jnp.zeros((TILES,), jnp.int32).at[grid_row * GRID_W + grid_col].set(jnp.arange(TILES, dtype=jnp.int32))
    columns = []
    for row_step in (-1, 0, 1):
        for col_step in (-1, 0, 1):
            if row_step == 0 and col_step == 0:
                continue
            near_row = grid_row + row_step
            near_col = grid_col + col_step
            inside = (near_row >= 0) & (near_row < GH) & (near_col >= 0) & (near_col < GRID_W)
            target = placed[jnp.clip(near_row, 0, GH - 1) * GRID_W + jnp.clip(near_col, 0, GRID_W - 1)]
            columns.append(jnp.where(inside, target, TILES))
    return jnp.stack(columns, axis=1).astype(jnp.int32)


def draw_valid_frames(key, part):
    grid_row = tile_layout(key)[0]
    cut_key = jax.random.fold_in(key, 103)
    top_cut = jax.random.randint(jax.random.fold_in(cut_key, 1), (), 0, GH // 4 + 1)
    bottom_cut = jax.random.randint(jax.random.fold_in(cut_key, 2), (), 0, GH // 4 + 1)
    in_band = (grid_row >= top_cut) & (grid_row < GH - bottom_cut)
    lengths = jax.random.randint(jax.random.fold_in(key, 104), (TILES,), 1, F + 1)
    whole_track = jax.random.randint(jax.random.fold_in(key, 105), (TILES,), 0, 2) == 1
    frame_counts = jnp.where(whole_track, F, lengths)
    return jnp.where(in_band, frame_counts, 0).astype(jnp.int32)


def block_scale(stream_key, dims, cuts, smallest, high):
    def one(position, shards_of):
        steps = jax.random.uniform(jax.random.fold_in(jax.random.fold_in(stream_key, 6), position), (shards_of,), jnp.float32, smallest / len(cuts), high / len(cuts))
        return jnp.repeat(jnp.exp(steps), dims[position] // shards_of).reshape((-1,) + (1,) * (len(dims) - position - 1))

    loudness = one(*cuts[0])
    for cut in cuts[1:]:
        loudness = loudness * one(*cut)
    return loudness


def centred(key, extent, deviation, most, cuts=(), kind=jnp.bfloat16):
    entries = deviation * jax.random.normal(key, extent, jnp.float32)
    if cuts:
        entries = entries * block_scale(key, extent, cuts, -0.22, 0.18)
    return jnp.clip(entries, -most, most).astype(kind)


def setup_inputs(seed: int = 0) -> dict:
    arg_keys = jax.random.split(jax.random.key(seed), 10)
    video_in = centred(arg_keys[0], (F, TILES, TS, TS * C), 1.0, 6.0, ((0, 8), (1, 32)))
    neighbours = draw_neighbours(jax.random.fold_in(arg_keys[9], 71), 0)
    valid_frames = draw_valid_frames(jax.random.fold_in(arg_keys[9], 71), 0)
    norm1_gain = jnp.clip(1.0 + 0.18 * jax.random.normal(arg_keys[3], (C,), jnp.float32), 0.1, 1.9)
    conv1_weight = centred(arg_keys[4], (9, 3 * C, C), (27 * C) ** -0.5, 0.078125)
    conv1_bias = centred(arg_keys[5], (C,), 0.5, 3.0, (), jnp.float32)
    norm2_gain = jnp.clip(1.0 + 0.18 * jax.random.normal(arg_keys[6], (C,), jnp.float32), 0.1, 1.9)
    conv2_weight = centred(arg_keys[7], (9, 3 * C, C), (27 * C) ** -0.5, 0.078125)
    conv2_bias = centred(arg_keys[8], (C,), 0.5, 3.0, (), jnp.float32)
    return dict(video_in=video_in, neighbours=neighbours, valid_frames=valid_frames, norm1_gain=norm1_gain, conv1_weight=conv1_weight, conv1_bias=conv1_bias, norm2_gain=norm2_gain, conv2_weight=conv2_weight, conv2_bias=conv2_bias)


epsilon = 1e-06

def norm_silu(values, scale_gain):
    square = lax.optimization_barrier(jnp.mean(values * values, axis=-1, keepdims=True))
    return jax.nn.silu(values * lax.rsqrt(square + epsilon) * scale_gain)

def conv_tile(framed, weight):
    frames_out = framed.shape[0] - 2
    side_len = framed.shape[1] - 2
    channels = framed.shape[-1]
    widened = jnp.concatenate([framed[:, :, col_off:col_off + side_len] for col_off in range(3)], axis=-1)
    summed = jnp.zeros((frames_out * side_len * side_len, channels), jnp.float32)
    for time_off in range(3):
        for row_off in range(3):
            window = widened[time_off:time_off + frames_out, row_off:row_off + side_len].reshape(-1, 3 * channels)
            summed = summed + jnp.dot(window, weight[time_off * 3 + row_off], preferred_element_type=jnp.float32)
    return summed.reshape(frames_out, side_len, side_len, channels)

def extend_tile(activation, tile_index, neighbours):
    nearby = lax.dynamic_index_in_dim(neighbours, tile_index, 0, keepdims=False)

    def fetch_tile(direction):
        other_tile = nearby[direction]
        fetched = lax.dynamic_index_in_dim(activation, jnp.minimum(other_tile, TILES - 1).astype(jnp.int32), 1, keepdims=False)
        return fetched * (other_tile < TILES).astype(activation.dtype)
    centre = lax.dynamic_index_in_dim(activation, tile_index, 1, keepdims=False)
    top_row = jnp.concatenate([fetch_tile(0)[:, -1:, -1:], fetch_tile(1)[:, -1:, :], fetch_tile(2)[:, -1:, :1]], axis=2)
    middle = jnp.concatenate([fetch_tile(3)[:, :, -1:], centre, fetch_tile(4)[:, :, :1]], axis=2)
    bottom_row = jnp.concatenate([fetch_tile(5)[:, :1, -1:], fetch_tile(6)[:, :1, :], fetch_tile(7)[:, :1, :1]], axis=2)
    framed = jnp.concatenate([top_row, middle, bottom_row], axis=1)
    return jnp.pad(framed, ((2, 0), (0, 0), (0, 0), (0, 0)))

def reference(video_in, neighbours, valid_frames, norm1_gain, conv1_weight, conv1_bias, norm2_gain, conv2_weight, conv2_bias):
    voxels = video_in.reshape(F, TILES, TS, TS, C)
    frame_ids = jnp.arange(F, dtype=jnp.int32)
    present = frame_ids[:, None] < valid_frames[None, :]
    masked = voxels * present[:, :, None, None, None].astype(voxels.dtype)
    activation = norm_silu(masked.astype(jnp.float32), norm1_gain).astype(jnp.bfloat16)
    tile_range = jnp.arange(TILES, dtype=jnp.int32)

    def frame_weights(tile_index):
        return lax.dynamic_index_in_dim(present, tile_index, 1, keepdims=False).astype(jnp.float32)[:, None, None, None]

    def first_pass(tile_index):
        summed = conv_tile(extend_tile(activation, tile_index, neighbours), conv1_weight)
        return norm_silu((summed + conv1_bias) * frame_weights(tile_index), norm2_gain).astype(jnp.bfloat16)
    hidden = jnp.moveaxis(lax.map(first_pass, tile_range), 0, 1)

    def second_pass(tile_index):
        summed = conv_tile(extend_tile(hidden, tile_index, neighbours), conv2_weight)
        residual = lax.dynamic_index_in_dim(masked, tile_index, 1, keepdims=False).astype(jnp.float32)
        return ((summed + conv2_bias) * frame_weights(tile_index) + residual).astype(jnp.bfloat16)
    block_out = jnp.moveaxis(lax.map(second_pass, tile_range), 0, 1)
    return block_out.reshape(F, TILES, TS, TS * C)
```

```python
import functools

import jax
import jax.numpy as jnp
from jax import lax
from jax.experimental import pallas as pl
from jax.experimental.pallas import tpu as pltpu
from jax.sharding import PartitionSpec as P

EPS = 1e-06
BF = jnp.bfloat16
F32 = jnp.float32
NT = 32
TM = 8
C = 192
L = 2 * C


def chunk_of(dev):
    z, y = lax.div(dev, 4), lax.rem(dev, 4)
    strip = lax.rem(y, 2) * 2 + lax.div(y, 2)
    return strip * 8 + lax.rem(3 * (z + 16 - 2 * strip), 8)


def device_of(chunk):
    strip, low = chunk // 8, chunk % 8
    return ((3 * low + 2 * strip) % 8) * 4 + (strip % 2) * 2 + strip // 2


def lanes(shape):
    return lax.broadcasted_iota(jnp.int32, shape, len(shape) - 1)


def rows(shape):
    return lax.broadcasted_iota(jnp.int32, shape, len(shape) - 2)


def norm_silu(v, gain):
    sq = v * v
    low = lanes((v.shape[0], 128)) < 64
    mid = sq[:, 128:256]
    zero = jnp.zeros_like(mid)
    first = jnp.sum(sq[:, :128] + jnp.where(low, mid, zero), axis=-1, keepdims=True)
    second = jnp.sum(sq[:, 256:] + jnp.where(low, zero, mid), axis=-1, keepdims=True)
    first = lax.rsqrt(first * (1.0 / C) + EPS)
    second = lax.rsqrt(second * (1.0 / C) + EPS)
    y = v * jnp.where(lanes(v.shape) < C, first, second) * gain
    half = 0.5 * y
    return half + half * jnp.tanh(half)


def down(v, first_row):
    return jnp.where(rows(v.shape) == 0, first_row, pltpu.roll(v, 1, 0))


def up(v, last_row):
    n = v.shape[0]
    return jnp.where(rows(v.shape) == n - 1, last_row, pltpu.roll(v, n - 1, 0))


def kernel(
    video, nbr, vf, g1, w1, b1, g2, w2, b2, out,
    vid, wr1, wr2, wt1, wt2, act, strip32, snd, got1, snd2, got2, gotc,
    pact, psnd, pgot, pgotc, ring, acc, racc, hid, hring, phid, phring, obuf,
    lsem, s1, r1, s2, r2, sc, rc, st, rt,
):
    t, s = lax.axis_index("tm"), lax.axis_index("space")
    nxt, prv = lax.rem(t + 1, TM), lax.rem(t + TM - 1, TM)

    barrier = pltpu.get_barrier_semaphore()

    def greet(k, carry):
        pl.semaphore_signal(barrier, inc=1, device_id={"space": lax.rem(s + k, NT)})
        return carry

    lax.fori_loop(1, NT, greet, 0)
    pl.semaphore_signal(barrier, inc=1, device_id={"tm": nxt})
    pl.semaphore_signal(barrier, inc=1, device_id={"tm": prv})

    load_v = pltpu.make_async_copy(video.at[:, 0], vid, lsem.at[0])
    load_v.start()
    load_1 = pltpu.make_async_copy(w1, wr1, lsem.at[1])
    load_1.start()
    load_2 = pltpu.make_async_copy(w2, wr2, lsem.at[2])
    load_2.start()

    def twice(ref):
        one = ref[...].reshape(1, C)
        return jnp.concatenate([one, one], axis=1)

    gain1, bias1, gain2, bias2 = twice(g1), twice(b1), twice(g2), twice(b2)
    first_frame = 4 * t
    own_valid = vf[s]

    def valid_of(k):
        n = nbr[s, k]
        return jnp.where(n < NT, vf[jnp.minimum(n, NT - 1)], 0)

    near = [valid_of(k) for k in range(8)]
    zero_row = jnp.zeros((1, L), F32)

    load_v.wait()
    for f in range(4):
        there = first_frame + f < own_valid
        for m in range(8):
            a = norm_silu(vid[f, :, L * m : L * m + L].astype(F32), gain1)
            a = jnp.where(there, a, 0.0)
            act[1, m + 1, f + 2] = a.astype(BF)
            act[0, m + 1, f + 2] = down(a, zero_row).astype(BF)
            act[2, m + 1, f + 2] = up(a, zero_row).astype(BF)
            strip32[m, f : f + 1] = a[0:1]
            strip32[m, 4 + f : 5 + f] = a[1:2]
            strip32[8 + m, f : f + 1] = a[14:15]
            strip32[8 + m, 4 + f : 5 + f] = a[15:16]
            if m in (0, 7):
                base = (16 if m == 0 else 24) + 2 * f
                snd[base] = a[0:8].astype(BF)
                snd[base + 1] = a[8:16].astype(BF)
    for c in range(16):
        snd[c] = strip32[c].astype(BF)
    got1[NT] = jnp.zeros((8, L), BF)

    pl.semaphore_wait(barrier, NT + 1)

    def send_1(k):
        j = lax.rem(s + k, NT)
        return pltpu.make_async_remote_copy(
            snd.at[chunk_of(j)], got1.at[s], s1.at[k], r1.at[k], device_id={"space": j}
        )

    def start_1(k, carry):
        send_1(k).start()
        return carry

    lax.fori_loop(1, NT, start_1, 0)
    got1[s] = snd[chunk_of(s)]

    def to_next(i, src, dst):
        return pltpu.make_async_remote_copy(src, dst, st.at[i], rt.at[i], device_id={"tm": nxt})

    t_act = to_next(0, act.at[1, 1:9, 4:6], pact)
    t_act.start()
    t_snd = to_next(1, snd.at[0:16], psnd)
    t_snd.start()

    def toeplitz(i, raw, wide):
        zeros = jnp.zeros((C, C), BF)
        for b in range(4):
            left = raw[i, b * C : b * C + C] if b < 3 else zeros
            right = raw[i, b * C - C : b * C] if b > 0 else zeros
            wide[i, b * C : b * C + C] = jnp.concatenate([left, right], axis=1)

    load_1.wait()

    def widen_1(i, carry):
        toeplitz(i, wr1, wt1)
        return carry

    lax.fori_loop(0, 9, widen_1, 0)

    def recv_1(k, carry):
        i = lax.rem(s + NT - k, NT)
        pltpu.make_async_remote_copy(
            snd.at[0], got1.at[i], s1.at[k], r1.at[k], device_id={"space": i}
        ).wait_recv()
        return carry

    lax.fori_loop(1, NT, recv_1, 0)
    mine = chunk_of(s)
    strip = lax.div(mine, 8)
    side = jnp.where(strip == 0, 6, jnp.where(strip == 1, 1, jnp.where(strip == 2, 4, 3)))
    is_corner = (mine == 0) | (mine == 7) | (mine == 8) | (mine == 15)
    corner = lax.div(mine + 1, 4) - 2 * lax.div(mine, 8)
    corner = lax.div(corner, 2) + 2 * lax.div(mine, 8)
    corner = lax.rem(corner, 4)
    cside = jnp.where(mine == 0, 7, jnp.where(mine == 7, 5, jnp.where(mine == 8, 2, 0)))

    def pick(d, carry):
        snd2[0, d] = got1[nbr[d, side]]
        snd2[1, d] = got1[nbr[d, cside]]
        return carry

    lax.fori_loop(0, NT, pick, 0)

    def send_2(k):
        d = lax.rem(s + k, NT)
        return pltpu.make_async_remote_copy(
            snd2.at[0, d], got2.at[mine], s2.at[k], r2.at[k], device_id={"space": d}
        )

    def send_c(k):
        d = lax.rem(s + k, NT)
        return pltpu.make_async_remote_copy(
            snd2.at[1, d], gotc.at[corner], sc.at[k], rc.at[corner], device_id={"space": d}
        )

    def start_2(k, carry):
        send_2(k).start()
        return carry

    lax.fori_loop(1, NT, start_2, 0)
    got2[mine] = snd2[0, s]

    @pl.when(is_corner)
    def _():
        def start_c(k, carry):
            send_c(k).start()
            return carry

        lax.fori_loop(1, NT, start_c, 0)
        gotc[corner] = snd2[1, s]

    later = t > 0
    t_act.wait_recv()

    def before(m, carry):
        for f in range(2):
            a = jnp.where(later, pact[m, f].astype(F32), 0.0)
            act[1, m + 1, f] = a.astype(BF)
            act[0, m + 1, f] = down(a, zero_row).astype(BF)
            act[2, m + 1, f] = up(a, zero_row).astype(BF)
        return carry

    lax.fori_loop(0, 8, before, 0)

    total = jnp.zeros((7 * 64, L), F32)
    for p in range(3):
        for q in range(3):
            window = jnp.concatenate(
                [act[q, 1:8, p : p + 4].reshape(-1, L), act[q, 2:9, p : p + 4].reshape(-1, L)],
                axis=1,
            )
            total = total + jnp.dot(window, wt1[3 * p + q], preferred_element_type=F32)
    acc[1:8] = total.reshape(7, 4, 16, L)

    load_2.wait()

    def widen_2(i, carry):
        toeplitz(i, wr2, wt2)
        return carry

    lax.fori_loop(0, 9, widen_2, 0)

    def recv_2(k, carry):
        i = lax.rem(s + NT - k, NT)
        pltpu.make_async_remote_copy(
            snd2.at[0, 0], got2.at[chunk_of(i)], s2.at[k], r2.at[k], device_id={"space": i}
        ).wait_recv()
        return carry

    lax.fori_loop(1, NT, recv_2, 0)
    for i, c in enumerate((0, 7, 8, 15)):

        @pl.when(mine != c)
        def _():
            pltpu.make_async_remote_copy(
                snd2.at[1, 0], gotc.at[i], sc.at[0], rc.at[i], device_id={"space": device_of(c)}
            ).wait_recv()

    t_got = [
        to_next(2, got2.at[0:16], pgot.at[0:16]),
        to_next(3, got2.at[20:24], pgot.at[16:20]),
        to_next(4, got2.at[28:32], pgot.at[20:24]),
        to_next(5, gotc, pgotc),
    ]
    for copy in t_got:
        copy.start()

    def side_pair(m, f, pieces):
        a = jnp.concatenate([pieces[0], pieces[1]], axis=0)
        act[1, m, f] = a.astype(BF)
        act[0, m, f] = down(a, zero_row).astype(BF)
        act[2, m, f] = up(a, zero_row).astype(BF)
        return a

    r8 = rows((8, L))

    def keep(v):
        return jnp.where(later, v, 0.0)

    edges = {}
    for m, base in ((0, 24), (9, 16)):
        mixed = jnp.zeros((8, L), F32)
        for f in range(4):
            pieces = [got2[base + 2 * f + h].astype(F32) for h in range(2)]
            side_pair(m, f + 2, pieces)
            mixed = jnp.where(r8 == f, pieces[0][0:1], mixed)
            mixed = jnp.where(r8 == 4 + f, pieces[1][7:8], mixed)
        edges[m] = mixed
    for copy in t_got:
        copy.wait_recv()
    t_snd.wait_recv()
    pedges = {}
    for m, base in ((0, 20), (9, 16)):
        mixed = jnp.zeros((8, L), F32)
        for f in range(2):
            pieces = [keep(pgot[base + 2 * f + h].astype(F32)) for h in range(2)]
            side_pair(m, f, pieces)
            mixed = jnp.where(r8 == 2 + f, pieces[0][0:1], mixed)
            mixed = jnp.where(r8 == 6 + f, pieces[1][7:8], mixed)
        pedges[m] = mixed

    def at_frames(p, prev, own):
        if p == 2:
            return own
        n = 2 - p
        return jnp.where(lax.rem(r8, 4) < n, pltpu.roll(prev, 4 + n, 0), pltpu.roll(own, n, 0))

    upper = r8 < 4
    none = jnp.zeros((8, L), F32)

    def ring_rows(m, top, bottom, inner, ptop, pbottom, pinner):
        for p in range(3):
            xt = at_frames(p, ptop, top)
            xb = at_frames(p, pbottom, bottom)
            xo = at_frames(p, pinner, inner)
            xt4, xb4 = pltpu.roll(xt, 4, 0), pltpu.roll(xb, 4, 0)
            tiles = (
                (jnp.where(upper, xt, xo), jnp.where(upper, xt4, none)),
                (jnp.where(upper, xt4, xb4), none),
                (jnp.where(upper, xo, xb), jnp.where(upper, none, xb4)),
            )
            for q in range(3):
                ring[3 * p + q, m] = jnp.concatenate(tiles[q], axis=0).astype(BF)

    def wide(ref, i):
        return ref[i].astype(F32)

    def ring_pair(m, carry):
        inner = jnp.where(upper, wide(snd, m), wide(snd, 8 + m))
        pinner = keep(jnp.where(upper, wide(psnd, m), wide(psnd, 8 + m)))
        ring_rows(
            m + 1, wide(got2, 8 + m), wide(got2, m), inner,
            keep(wide(pgot, 8 + m)), keep(wide(pgot, m)), pinner,
        )
        return carry

    lax.fori_loop(0, 8, ring_pair, 0)
    ring_rows(
        0, wide(gotc, 3), wide(gotc, 1), edges[0],
        keep(wide(pgotc, 3)), keep(wide(pgotc, 1)), pedges[0],
    )
    ring_rows(
        9, wide(gotc, 2), wide(gotc, 0), edges[9],
        keep(wide(pgotc, 2)), keep(wide(pgotc, 0)), pedges[9],
    )

    total = jnp.zeros((2 * 64 + 9 * 16, L), F32)
    for p in range(3):
        for q in range(3):
            halves = []
            for d in range(2):
                halves.append(
                    jnp.concatenate(
                        [
                            act[q, d, p : p + 4].reshape(-1, L),
                            act[q, 8 + d, p : p + 4].reshape(-1, L),
                            ring[3 * p + q, d : d + 9].reshape(-1, L),
                        ],
                        axis=0,
                    )
                )
            window = jnp.concatenate(halves, axis=1)
            total = total + jnp.dot(window, wt1[3 * p + q], preferred_element_type=F32)
    acc[0] = total[0:64].reshape(4, 16, L)
    acc[8] = total[64:128].reshape(4, 16, L)
    racc[...] = total[128:].reshape(9, 16, L)

    def finish(m, carry):
        rim = racc[m]
        left_half = lanes((8, L)) < C

        def by_pair(left, middle, right):
            first = jnp.where(m == 0, left, middle)
            second = jnp.where(m == 8, right, middle)
            return first, second

        t0, t1 = by_pair(near[0], near[1], near[2])
        u0, u1 = by_pair(near[5], near[6], near[7])
        o0, o1 = by_pair(near[3], own_valid, near[4])
        limit = jnp.where(upper, jnp.where(left_half, t0, t1), jnp.where(left_half, u0, u1))
        outer = norm_silu(rim[0:8] + bias1, gain2)
        outer = jnp.where(first_frame + lax.rem(r8, 4) < limit, outer, 0.0)
        hring[m] = outer.astype(BF)
        limit = jnp.where(lanes((16, L)) < C, o0, o1)
        r16 = rows((16, L))
        for f in range(4):
            v = acc[m, f]
            v = v + jnp.where(r16 == 0, rim[8 + f : 9 + f], 0.0)
            v = v + jnp.where(r16 == 15, rim[12 + f : 13 + f], 0.0)
            h = norm_silu(v + bias1, gain2)
            h = jnp.where(first_frame + f < limit, h, 0.0)
            hid[1, m, f + 2] = h.astype(BF)
            hid[0, m, f + 2] = down(h, outer[f : f + 1]).astype(BF)
            hid[2, m, f + 2] = up(h, outer[4 + f : 5 + f]).astype(BF)
        return carry

    lax.fori_loop(0, 9, finish, 0)
    t_hid = [to_next(6, hid.at[1, :, 4:6], phid), to_next(7, hring, phring)]
    for copy in t_hid:
        copy.start()

    def conv2(half):
        total = jnp.zeros((8 * 32, L), F32)
        for p in range(3):
            for q in range(3):
                f = 2 * half + p
                window = jnp.concatenate(
                    [hid[q, 0:8, f : f + 2].reshape(-1, L), hid[q, 1:9, f : f + 2].reshape(-1, L)],
                    axis=1,
                )
                total = total + jnp.dot(window, wt2[3 * p + q], preferred_element_type=F32)
        total = total.reshape(8, 2, 16, L)
        for g in range(2):
            f = 2 * half + g
            there = first_frame + f < own_valid
            for m in range(8):
                x = vid[f, :, L * m : L * m + L].astype(F32)
                o = jnp.where(there, total[m, g] + bias2 + x, 0.0)
                obuf[f, :, L * m : L * m + L] = o.astype(BF)
        copy = pltpu.make_async_copy(
            obuf.at[2 * half : 2 * half + 2], out.at[2 * half : 2 * half + 2, 0], lsem.at[3 + half]
        )
        copy.start()
        return copy

    store_1 = conv2(1)
    for copy in t_hid:
        copy.wait_recv()

    def before_2(m, carry):
        rim = keep(phring[m].astype(F32))
        for f in range(2):
            h = keep(phid[m, f].astype(F32))
            hid[1, m, f] = h.astype(BF)
            hid[0, m, f] = down(h, rim[2 + f : 3 + f]).astype(BF)
            hid[2, m, f] = up(h, rim[6 + f : 7 + f]).astype(BF)
        return carry

    lax.fori_loop(0, 9, before_2, 0)
    store_0 = conv2(0)

    def sent(k, carry):
        send_1(k).wait_send()
        send_2(k).wait_send()
        return carry

    lax.fori_loop(1, NT, sent, 0)

    @pl.when(is_corner)
    def _():
        def sent_c(k, carry):
            send_c(k).wait_send()
            return carry

        lax.fori_loop(1, NT, sent_c, 0)

    for copy in [t_act, t_snd, *t_got, *t_hid]:
        copy.wait_send()
    store_1.wait()
    store_0.wait()


def on_device(video, nbr, vf, g1, w1, b1, g2, w2, b2):
    vmem = lambda *shape, dtype=BF: pltpu.VMEM(shape, dtype)
    dma = lambda n: pltpu.SemaphoreType.DMA((n,))
    hbm = pl.BlockSpec(memory_space=pl.ANY)
    smem = pl.BlockSpec(memory_space=pltpu.SMEM)
    local = pl.BlockSpec(memory_space=pltpu.VMEM)
    return pl.pallas_call(
        kernel,
        out_shape=jax.ShapeDtypeStruct(video.shape, BF),
        in_specs=[hbm, smem, smem, local, hbm, local, local, hbm, local],
        out_specs=hbm,
        scratch_shapes=[
            vmem(4, 16, 16 * C),
            vmem(9, 3 * C, C),
            vmem(9, 3 * C, C),
            vmem(9, 4 * C, L),
            vmem(9, 4 * C, L),
            vmem(3, 10, 6, 16, L),
            vmem(16, 8, L, dtype=F32),
            vmem(32, 8, L),
            vmem(NT + 1, 8, L),
            vmem(2, NT, 8, L),
            vmem(32, 8, L),
            vmem(4, 8, L),
            vmem(8, 2, 16, L),
            vmem(16, 8, L),
            vmem(24, 8, L),
            vmem(4, 8, L),
            vmem(9, 10, 16, L),
            vmem(9, 4, 16, L, dtype=F32),
            vmem(9, 16, L, dtype=F32),
            vmem(3, 9, 6, 16, L),
            vmem(9, 8, L),
            vmem(9, 2, 16, L),
            vmem(9, 8, L),
            vmem(4, 16, 16 * C),
            dma(5), dma(NT), dma(NT), dma(NT), dma(NT), dma(NT), dma(4), dma(8), dma(8),
        ],
        compiler_params=pltpu.CompilerParams(
            collective_id=0, has_side_effects=True, vmem_limit_bytes=60 * 1024 * 1024
        ),
    )(video, nbr, vf, g1, w1, b1, g2, w2, b2)


def solution(mesh):
    placed = (P("tm", "space", None, None), P(), P(), P(), P(), P(), P(), P(), P())
    return jax.shard_map(
        on_device, mesh=mesh, in_specs=placed, out_specs=P("tm", "space", None, None), check_vma=False
    )
```

```python
import functools

import jax
import jax.numpy as jnp
from jax import lax
from jax.experimental import pallas as pl
from jax.experimental.pallas import tpu as pltpu
from jax.sharding import PartitionSpec as P

EPS = 1e-06
BF = jnp.bfloat16
F32 = jnp.float32
NT = 32
TM = 8
C = 192
L = 2 * C


def chunk_of(dev):
    z, y = lax.div(dev, 4), lax.rem(dev, 4)
    strip = lax.rem(y, 2) * 2 + lax.div(y, 2)
    return strip * 8 + lax.rem(3 * (z + 16 - 2 * strip), 8)


def device_of(chunk):
    strip, low = chunk // 8, chunk % 8
    return ((3 * low + 2 * strip) % 8) * 4 + (strip % 2) * 2 + strip // 2


def lanes(shape):
    return lax.broadcasted_iota(jnp.int32, shape, len(shape) - 1)


def rows(shape):
    return lax.broadcasted_iota(jnp.int32, shape, len(shape) - 2)


def norm_silu(v, gain):
    sq = v * v
    low = lanes((v.shape[0], 128)) < 64
    mid = sq[:, 128:256]
    zero = jnp.zeros_like(mid)
    first = jnp.sum(sq[:, :128] + jnp.where(low, mid, zero), axis=-1, keepdims=True)
    second = jnp.sum(sq[:, 256:] + jnp.where(low, zero, mid), axis=-1, keepdims=True)
    first = lax.rsqrt(first * (1.0 / C) + EPS)
    second = lax.rsqrt(second * (1.0 / C) + EPS)
    y = v * jnp.where(lanes(v.shape) < C, first, second) * gain
    half = 0.5 * y
    return half + half * jnp.tanh(half)


def matmul(a, b):
    return lax.dot_general(a, b, (((1,), (1,)), ((), ())), preferred_element_type=F32)


def down(v, first_row):
    return jnp.where(rows(v.shape) == 0, first_row, pltpu.roll(v, 1, 0))


def up(v, last_row):
    n = v.shape[0]
    return jnp.where(rows(v.shape) == n - 1, last_row, pltpu.roll(v, n - 1, 0))


def kernel(
    video, nbr_in, vf_in, g1_in, w1, b1_in, g2_in, w2, b2_in, out,
    nbr, vf, g1, b1, g2, b2, vid, wr1, wr2, wt1, wt2, act, strip32, snd, got1, snd2, got2, gotc,
    pact, psnd, pgot, pgotc, ring, acc, racc, hid, hring, phid, phring,
    lsem, s1, r1, s2, r2, sc, rc, st, rt,
):
    t, s = lax.axis_index("tm"), lax.axis_index("space")
    nxt, prv = lax.rem(t + 1, TM), lax.rem(t + TM - 1, TM)

    barrier = pltpu.get_barrier_semaphore()

    def greet(k, carry):
        pl.semaphore_signal(barrier, inc=1, device_id={"space": lax.rem(s + k, NT)})
        return carry

    lax.fori_loop(1, NT, greet, 0)
    pl.semaphore_signal(barrier, inc=1, device_id={"tm": nxt})
    pl.semaphore_signal(barrier, inc=1, device_id={"tm": prv})

    loads = [
        pltpu.make_async_copy(src, dst, lsem.at[3 + i])
        for i, (src, dst) in enumerate(
            ((nbr_in, nbr), (vf_in, vf), (g1_in, g1), (b1_in, b1), (g2_in, g2), (b2_in, b2))
        )
    ]
    for copy in loads:
        copy.start()
    load_v = pltpu.make_async_copy(video.at[:, 0], vid, lsem.at[0])
    load_v.start()
    load_1 = pltpu.make_async_copy(w1, wr1, lsem.at[1])
    load_1.start()
    load_2 = pltpu.make_async_copy(w2, wr2, lsem.at[2])
    load_2.start()

    for copy in loads:
        copy.wait()

    def twice(ref):
        one = ref[...].reshape(1, C)
        return jnp.concatenate([one, one], axis=1)

    gain1, bias1, gain2, bias2 = twice(g1), twice(b1), twice(g2), twice(b2)
    first_frame = 4 * t
    own_valid = vf[s]

    def valid_of(k):
        n = nbr[k, s]
        return jnp.where(n < NT, vf[jnp.minimum(n, NT - 1)], 0)

    near = [valid_of(k) for k in range(8)]
    zero_row = jnp.zeros((1, L), F32)

    load_v.wait()
    for f in range(4):
        there = first_frame + f < own_valid
        for m in range(8):
            a = norm_silu(vid[f, :, L * m : L * m + L].astype(F32), gain1)
            a = jnp.where(there, a, 0.0)
            act[1, m + 1, f + 2] = a.astype(BF)
            act[0, m + 1, f + 2] = down(a, zero_row).astype(BF)
            act[2, m + 1, f + 2] = up(a, zero_row).astype(BF)
            strip32[m, f : f + 1] = a[0:1]
            strip32[m, 4 + f : 5 + f] = a[1:2]
            strip32[8 + m, f : f + 1] = a[14:15]
            strip32[8 + m, 4 + f : 5 + f] = a[15:16]
            if m in (0, 7):
                base = (16 if m == 0 else 24) + 2 * f
                snd[base] = a[0:8].astype(BF)
                snd[base + 1] = a[8:16].astype(BF)
    for c in range(16):
        snd[c] = strip32[c].astype(BF)
    got1[NT] = jnp.zeros((8, L), BF)

    pl.semaphore_wait(barrier, NT + 1)

    def send_1(k):
        j = lax.rem(s + k, NT)
        return pltpu.make_async_remote_copy(
            snd.at[chunk_of(j)], got1.at[s], s1.at[k], r1.at[k], device_id={"space": j}
        )

    def start_1(k, carry):
        send_1(k).start()
        return carry

    lax.fori_loop(1, NT, start_1, 0)
    got1[s] = snd[chunk_of(s)]

    def to_next(i, src, dst):
        return pltpu.make_async_remote_copy(src, dst, st.at[i], rt.at[i], device_id={"tm": nxt})

    t_act = to_next(0, act.at[1, 1:9, 4:6], pact)
    t_act.start()
    t_snd = to_next(1, snd.at[0:16], psnd)
    t_snd.start()

    def toeplitz(i, raw, wide):
        zeros = jnp.zeros((C, C), BF)
        one = raw[i]
        wide[i, 0:C] = jnp.concatenate([one, zeros], axis=1)
        wide[i, C:L] = jnp.concatenate([zeros, one], axis=1)

    load_1.wait()

    def widen_1(i, carry):
        toeplitz(i, wr1, wt1)
        return carry

    lax.fori_loop(0, 9, widen_1, 0)

    def recv_1(k, carry):
        i = lax.rem(s + NT - k, NT)
        pltpu.make_async_remote_copy(
            snd.at[0], got1.at[i], s1.at[k], r1.at[k], device_id={"space": i}
        ).wait_recv()
        return carry

    lax.fori_loop(1, NT, recv_1, 0)
    mine = chunk_of(s)
    strip = lax.div(mine, 8)
    side = jnp.where(strip == 0, 6, jnp.where(strip == 1, 1, jnp.where(strip == 2, 4, 3)))
    is_corner = (mine == 0) | (mine == 7) | (mine == 8) | (mine == 15)
    corner = lax.rem(2 * strip + lax.div(lax.rem(mine, 8), 7), 4)
    cside = jnp.where(mine == 0, 7, jnp.where(mine == 7, 5, jnp.where(mine == 8, 2, 0)))

    def pick(d, carry):
        snd2[0, d] = got1[nbr[side, d]]
        snd2[1, d] = got1[nbr[cside, d]]
        return carry

    lax.fori_loop(0, NT, pick, 0)

    def send_2(k):
        d = lax.rem(s + k, NT)
        return pltpu.make_async_remote_copy(
            snd2.at[0, d], got2.at[mine], s2.at[k], r2.at[k], device_id={"space": d}
        )

    def send_c(k):
        d = lax.rem(s + k, NT)
        return pltpu.make_async_remote_copy(
            snd2.at[1, d], gotc.at[corner], sc.at[k], rc.at[corner], device_id={"space": d}
        )

    def start_2(k, carry):
        send_2(k).start()
        return carry

    lax.fori_loop(1, NT, start_2, 0)
    got2[mine] = snd2[0, s]

    @pl.when(is_corner)
    def _():
        def start_c(k, carry):
            send_c(k).start()
            return carry

        lax.fori_loop(1, NT, start_c, 0)
        gotc[corner] = snd2[1, s]

    later = t > 0
    t_act.wait_recv()

    def before(m, carry):
        for f in range(2):
            a = jnp.where(later, pact[m, f].astype(F32), 0.0)
            act[1, m + 1, f] = a.astype(BF)
            act[0, m + 1, f] = down(a, zero_row).astype(BF)
            act[2, m + 1, f] = up(a, zero_row).astype(BF)
        return carry

    lax.fori_loop(0, 8, before, 0)

    total = jnp.zeros((7 * 64, L), F32)
    for p in range(3):
        for q in range(3):
            window = jnp.concatenate(
                [act[q, 1:8, p : p + 4].reshape(-1, L), act[q, 2:9, p : p + 4].reshape(-1, L)],
                axis=1,
            )
            total = total + matmul(window, wt1[3 * p + q])
    acc[1:8] = total.reshape(7, 4, 16, L)

    load_2.wait()

    def widen_2(i, carry):
        toeplitz(i, wr2, wt2)
        return carry

    lax.fori_loop(0, 9, widen_2, 0)

    def recv_2(k, carry):
        i = lax.rem(s + NT - k, NT)
        pltpu.make_async_remote_copy(
            snd2.at[0, 0], got2.at[chunk_of(i)], s2.at[k], r2.at[k], device_id={"space": i}
        ).wait_recv()
        return carry

    lax.fori_loop(1, NT, recv_2, 0)
    for i, c in enumerate((0, 7, 8, 15)):

        @pl.when(mine != c)
        def _():
            pltpu.make_async_remote_copy(
                snd2.at[1, 0], gotc.at[i], sc.at[0], rc.at[i], device_id={"space": device_of(c)}
            ).wait_recv()

    t_got = [
        to_next(2, got2.at[0:16], pgot.at[0:16]),
        to_next(3, got2.at[20:24], pgot.at[16:20]),
        to_next(4, got2.at[28:32], pgot.at[20:24]),
        to_next(5, gotc, pgotc),
    ]
    for copy in t_got:
        copy.start()

    def side_pair(m, f, pieces):
        a = jnp.concatenate([pieces[0], pieces[1]], axis=0)
        act[1, m, f] = a.astype(BF)
        act[0, m, f] = down(a, zero_row).astype(BF)
        act[2, m, f] = up(a, zero_row).astype(BF)
        return a

    r8 = rows((8, L))

    def keep(v):
        return jnp.where(later, v, 0.0)

    edges = {}
    for m, base in ((0, 24), (9, 16)):
        mixed = jnp.zeros((8, L), F32)
        for f in range(4):
            pieces = [got2[base + 2 * f + h].astype(F32) for h in range(2)]
            side_pair(m, f + 2, pieces)
            mixed = jnp.where(r8 == f, pieces[0][0:1], mixed)
            mixed = jnp.where(r8 == 4 + f, pieces[1][7:8], mixed)
        edges[m] = mixed
    for copy in t_got:
        copy.wait_recv()
    t_snd.wait_recv()
    pedges = {}
    for m, base in ((0, 20), (9, 16)):
        mixed = jnp.zeros((8, L), F32)
        for f in range(2):
            pieces = [keep(pgot[base + 2 * f + h].astype(F32)) for h in range(2)]
            side_pair(m, f, pieces)
            mixed = jnp.where(r8 == 2 + f, pieces[0][0:1], mixed)
            mixed = jnp.where(r8 == 6 + f, pieces[1][7:8], mixed)
        pedges[m] = mixed

    def at_frames(p, prev, own):
        if p == 2:
            return own
        n = 2 - p
        return jnp.where(lax.rem(r8, 4) < n, pltpu.roll(prev, 4 + n, 0), pltpu.roll(own, n, 0))

    upper = r8 < 4
    none = jnp.zeros((8, L), F32)

    def ring_rows(m, top, bottom, inner, ptop, pbottom, pinner):
        for p in range(3):
            xt = at_frames(p, ptop, top)
            xb = at_frames(p, pbottom, bottom)
            xo = at_frames(p, pinner, inner)
            xt4, xb4 = pltpu.roll(xt, 4, 0), pltpu.roll(xb, 4, 0)
            tiles = (
                (jnp.where(upper, xt, xo), jnp.where(upper, xt4, none)),
                (jnp.where(upper, xt4, xb4), none),
                (jnp.where(upper, xo, xb), jnp.where(upper, none, xb4)),
            )
            for q in range(3):
                ring[3 * p + q, m] = jnp.concatenate(tiles[q], axis=0).astype(BF)

    def wide(ref, i):
        return ref[i].astype(F32)

    def ring_pair(m, carry):
        inner = jnp.where(upper, wide(snd, m), wide(snd, 8 + m))
        pinner = keep(jnp.where(upper, wide(psnd, m), wide(psnd, 8 + m)))
        ring_rows(
            m + 1, wide(got2, 8 + m), wide(got2, m), inner,
            keep(wide(pgot, 8 + m)), keep(wide(pgot, m)), pinner,
        )
        return carry

    lax.fori_loop(0, 8, ring_pair, 0)
    ring_rows(
        0, wide(gotc, 3), wide(gotc, 1), edges[0],
        keep(wide(pgotc, 3)), keep(wide(pgotc, 1)), pedges[0],
    )
    ring_rows(
        9, wide(gotc, 2), wide(gotc, 0), edges[9],
        keep(wide(pgotc, 2)), keep(wide(pgotc, 0)), pedges[9],
    )

    total = jnp.zeros((2 * 64 + 9 * 16, L), F32)
    for p in range(3):
        for q in range(3):
            halves = []
            for d in range(2):
                halves.append(
                    jnp.concatenate(
                        [
                            act[q, d, p : p + 4].reshape(-1, L),
                            act[q, 8 + d, p : p + 4].reshape(-1, L),
                            ring[3 * p + q, d : d + 9].reshape(-1, L),
                        ],
                        axis=0,
                    )
                )
            window = jnp.concatenate(halves, axis=1)
            total = total + matmul(window, wt1[3 * p + q])
    acc[0] = total[0:64].reshape(4, 16, L)
    acc[8] = total[64:128].reshape(4, 16, L)
    racc[...] = total[128:].reshape(9, 16, L)

    def finish(m, carry):
        rim = racc[m]
        left_half = lanes((8, L)) < C

        def by_pair(left, middle, right):
            first = jnp.where(m == 0, left, middle)
            second = jnp.where(m == 8, right, middle)
            return first, second

        t0, t1 = by_pair(near[0], near[1], near[2])
        u0, u1 = by_pair(near[5], near[6], near[7])
        o0, o1 = by_pair(near[3], own_valid, near[4])
        limit = jnp.where(upper, jnp.where(left_half, t0, t1), jnp.where(left_half, u0, u1))
        outer = norm_silu(rim[0:8] + bias1, gain2)
        outer = jnp.where(first_frame + lax.rem(r8, 4) < limit, outer, 0.0)
        hring[m] = outer.astype(BF)
        limit = jnp.where(lanes((16, L)) < C, o0, o1)
        r16 = rows((16, L))
        for f in range(4):
            v = acc[m, f]
            v = v + jnp.where(r16 == 0, rim[8 + f : 9 + f], 0.0)
            v = v + jnp.where(r16 == 15, rim[12 + f : 13 + f], 0.0)
            h = norm_silu(v + bias1, gain2)
            h = jnp.where(first_frame + f < limit, h, 0.0)
            hid[1, m, f + 2] = h.astype(BF)
            hid[0, m, f + 2] = down(h, outer[f : f + 1]).astype(BF)
            hid[2, m, f + 2] = up(h, outer[4 + f : 5 + f]).astype(BF)
        return carry

    lax.fori_loop(0, 9, finish, 0)
    t_hid = [to_next(6, hid.at[1, :, 4:6], phid), to_next(7, hring, phring)]
    for copy in t_hid:
        copy.start()

    def conv2(half):
        total = jnp.zeros((8 * 32, L), F32)
        for p in range(3):
            for q in range(3):
                f = 2 * half + p
                window = jnp.concatenate(
                    [hid[q, 0:8, f : f + 2].reshape(-1, L), hid[q, 1:9, f : f + 2].reshape(-1, L)],
                    axis=1,
                )
                total = total + matmul(window, wt2[3 * p + q])
        total = total.reshape(8, 2, 16, L)
        for g in range(2):
            f = 2 * half + g
            there = first_frame + f < own_valid
            for m in range(8):
                x = vid[f, :, L * m : L * m + L].astype(F32)
                o = jnp.where(there, total[m, g] + bias2 + x, 0.0)
                out[f, 0, :, L * m : L * m + L] = o.astype(BF)

    conv2(1)
    for copy in t_hid:
        copy.wait_recv()

    def before_2(m, carry):
        rim = keep(phring[m].astype(F32))
        for f in range(2):
            h = keep(phid[m, f].astype(F32))
            hid[1, m, f] = h.astype(BF)
            hid[0, m, f] = down(h, rim[2 + f : 3 + f]).astype(BF)
            hid[2, m, f] = up(h, rim[6 + f : 7 + f]).astype(BF)
        return carry

    lax.fori_loop(0, 9, before_2, 0)
    conv2(0)

    def sent(k, carry):
        send_1(k).wait_send()
        send_2(k).wait_send()
        return carry

    lax.fori_loop(1, NT, sent, 0)

    @pl.when(is_corner)
    def _():
        def sent_c(k, carry):
            send_c(k).wait_send()
            return carry

        lax.fori_loop(1, NT, sent_c, 0)

    for copy in [t_act, t_snd, *t_got, *t_hid]:
        copy.wait_send()


def on_device(video, nbr, vf, g1, w1, b1, g2, w2, b2):
    vmem = lambda *shape, dtype=BF: pltpu.VMEM(shape, dtype)
    dma = lambda n: pltpu.SemaphoreType.DMA((n,))
    hbm = pl.BlockSpec(memory_space=pltpu.HBM)
    local = pl.BlockSpec(memory_space=pltpu.VMEM)
    return pl.pallas_call(
        kernel,
        out_shape=pltpu.VMEM(video.shape, BF),
        in_specs=[hbm] * 9,
        out_specs=local,
        scratch_shapes=[
            pltpu.SMEM((8, NT), jnp.int32),
            pltpu.SMEM((NT,), jnp.int32),
            *[vmem(C, dtype=F32)] * 4,
            vmem(4, 16, 16 * C),
            vmem(9, C, 3 * C),
            vmem(9, C, 3 * C),
            vmem(9, L, 4 * C),
            vmem(9, L, 4 * C),
            vmem(3, 10, 6, 16, L),
            vmem(16, 8, L, dtype=F32),
            vmem(32, 8, L),
            vmem(NT + 1, 8, L),
            vmem(2, NT, 8, L),
            vmem(32, 8, L),
            vmem(4, 8, L),
            vmem(8, 2, 16, L),
            vmem(16, 8, L),
            vmem(24, 8, L),
            vmem(4, 8, L),
            vmem(9, 10, 16, L),
            vmem(9, 4, 16, L, dtype=F32),
            vmem(9, 16, L, dtype=F32),
            vmem(3, 9, 6, 16, L),
            vmem(9, 8, L),
            vmem(9, 2, 16, L),
            vmem(9, 8, L),
            dma(9), dma(NT), dma(NT), dma(NT), dma(NT), dma(NT), dma(4), dma(8), dma(8),
        ],
        compiler_params=pltpu.CompilerParams(
            collective_id=0, has_side_effects=True, vmem_limit_bytes=66000000
        ),
    )(video, nbr.T, vf, g1, jnp.swapaxes(w1, 1, 2), b1, g2, jnp.swapaxes(w2, 1, 2), b2)


def solution(mesh):
    placed = (P("tm", "space", None, None), P(), P(), P(), P(), P(), P(), P(), P())
    return jax.shard_map(
        on_device, mesh=mesh, in_specs=placed, out_specs=P("tm", "space", None, None), check_vma=False
    )
```

```python
import functools

import jax
import jax.numpy as jnp
from jax import lax
from jax.experimental import pallas as pl
from jax.experimental.pallas import tpu as pltpu
from jax.sharding import PartitionSpec as P

EPS = 1e-06
BF = jnp.bfloat16
F32 = jnp.float32
NT = 32
TM = 8
C = 192
L = 2 * C


def chunk_of(dev):
    z, y = lax.div(dev, 4), lax.rem(dev, 4)
    strip = lax.rem(y, 2) * 2 + lax.div(y, 2)
    return strip * 8 + lax.rem(3 * (z + 16 - 2 * strip), 8)


def device_of(chunk):
    strip, low = chunk // 8, chunk % 8
    return ((3 * low + 2 * strip) % 8) * 4 + (strip % 2) * 2 + strip // 2


def offset(i):
    return 16 + (1 - 2 * lax.rem(i, 2)) * lax.div(i + 1, 2)


def lanes(shape):
    return lax.broadcasted_iota(jnp.int32, shape, len(shape) - 1)


def rows(shape):
    return lax.broadcasted_iota(jnp.int32, shape, len(shape) - 2)


def norm_silu(v, gain):
    sq = v * v
    low = lanes((v.shape[0], 128)) < 64
    mid = sq[:, 128:256]
    zero = jnp.zeros_like(mid)
    first = jnp.sum(sq[:, :128] + jnp.where(low, mid, zero), axis=-1, keepdims=True)
    second = jnp.sum(sq[:, 256:] + jnp.where(low, zero, mid), axis=-1, keepdims=True)
    first = lax.rsqrt(first * (1.0 / C) + EPS)
    second = lax.rsqrt(second * (1.0 / C) + EPS)
    y = v * jnp.where(lanes(v.shape) < C, first, second) * gain
    half = 0.5 * y
    return half + half * jnp.tanh(half)


def matmul(a, b):
    return lax.dot_general(a, b, (((1,), (1,)), ((), ())), preferred_element_type=F32)


def conv_rows(windows, near_w, far_w):
    first = jnp.concatenate([w[:, : C + L + 64] for w in windows], axis=1)
    second = jnp.concatenate([w[:, 128:] for w in windows], axis=1)
    near_w = jnp.concatenate([near_w[i] for i in range(9)], axis=1)
    far_w = jnp.concatenate([far_w[i] for i in range(9)], axis=1)
    a, b = matmul(first, near_w), matmul(second, far_w)
    return jnp.concatenate([a[:, :128], a[:, 128:] + b[:, :128], b[:, 128:]], axis=1)


def down(v, first_row):
    return jnp.where(rows(v.shape) == 0, first_row, pltpu.roll(v, 1, 0))


def up(v, last_row):
    n = v.shape[0]
    return jnp.where(rows(v.shape) == n - 1, last_row, pltpu.roll(v, n - 1, 0))


def kernel(
    video, nbr_in, vf_in, g1_in, w1, b1_in, g2_in, w2, b2_in, out,
    nbr, vf, g1, b1, g2, b2, vid, wr1, wr2, near1, far1, near2, far2, act, strip32, snd, got1, snd2, got2,
    pact, psnd, pgot, inner, pinner, ring, acc, racc, hid, hring, phid, phring,
    lsem, s1, r1, s2, r2, sc, rc, st, rt,
):
    t, s = lax.axis_index("tm"), lax.axis_index("space")
    nxt, prv = lax.rem(t + 1, TM), lax.rem(t + TM - 1, TM)

    barrier = pltpu.get_barrier_semaphore()

    later, sends = t > 0, t < TM - 1

    def greet(i, carry):
        pl.semaphore_signal(barrier, inc=1, device_id={"space": lax.rem(s + offset(i), NT)})
        return carry

    lax.fori_loop(0, NT - 1, greet, 0)

    @pl.when(sends)
    def _():
        pl.semaphore_signal(barrier, inc=1, device_id={"tm": nxt})

    @pl.when(later)
    def _():
        pl.semaphore_signal(barrier, inc=1, device_id={"tm": prv})

    loads = [
        pltpu.make_async_copy(src, dst, lsem.at[3 + i])
        for i, (src, dst) in enumerate(
            ((nbr_in, nbr), (vf_in, vf), (g1_in, g1), (b1_in, b1), (g2_in, g2), (b2_in, b2))
        )
    ]
    for copy in loads:
        copy.start()
    load_v = pltpu.make_async_copy(video.at[:, 0], vid, lsem.at[0])
    load_v.start()
    load_1 = pltpu.make_async_copy(w1, wr1, lsem.at[1])
    load_1.start()
    load_2 = pltpu.make_async_copy(w2, wr2, lsem.at[2])
    load_2.start()

    for copy in loads:
        copy.wait()

    def twice(ref):
        one = ref[...].reshape(1, C)
        return jnp.concatenate([one, one], axis=1)

    gain1, bias1, gain2, bias2 = twice(g1), twice(b1), twice(g2), twice(b2)
    first_frame = 4 * t
    own_valid = vf[s]

    def valid_of(k):
        n = nbr[k, s]
        return jnp.where(n < NT, vf[jnp.minimum(n, NT - 1)], 0)

    near = [valid_of(k) for k in range(8)]
    zero_row = jnp.zeros((1, L), F32)

    load_v.wait()
    for f in range(4):
        there = first_frame + f < own_valid
        for m in range(8):
            a = norm_silu(vid[f, :, L * m : L * m + L].astype(F32), gain1)
            a = jnp.where(there, a, 0.0)
            act[1, m + 1, f + 2] = a.astype(BF)
            act[0, m + 1, f + 2] = down(a, zero_row).astype(BF)
            act[2, m + 1, f + 2] = up(a, zero_row).astype(BF)
            strip32[m, f : f + 1] = a[0:1]
            strip32[m, 4 + f : 5 + f] = a[1:2]
            strip32[8 + m, f : f + 1] = a[14:15]
            strip32[8 + m, 4 + f : 5 + f] = a[15:16]
            if m in (0, 7):
                base = (16 if m == 0 else 24) + 2 * f
                snd[base] = a[0:8].astype(BF)
                snd[base + 1] = a[8:16].astype(BF)
    for c in range(16):
        snd[c] = strip32[c].astype(BF)
    got1[NT] = jnp.zeros((8, L), BF)

    pl.semaphore_wait(barrier, NT - 1 + jnp.where(later, 1, 0) + jnp.where(sends, 1, 0))

    def send_1(k):
        j = lax.rem(s + k, NT)
        return pltpu.make_async_remote_copy(
            snd.at[chunk_of(j)], got1.at[s], s1.at[k], r1.at[k], device_id={"space": j}
        )

    def start_1(i, carry):
        send_1(offset(i)).start()
        return carry

    lax.fori_loop(0, NT - 1, start_1, 0)
    got1[s] = snd[chunk_of(s)]

    def to_next(i, src, dst):
        return pltpu.make_async_remote_copy(src, dst, st.at[i], rt.at[i], device_id={"tm": nxt})

    t_act = to_next(0, act.at[1, 1:9, 4:6], pact)
    t_snd = to_next(1, snd.at[0:16], psnd)

    @pl.when(sends)
    def _():
        t_act.start()
        t_snd.start()

    def widen(i, raw, near_w, far_w):
        one, pad = raw[i], jnp.zeros((C, 64), BF)
        near_w[i, 0:C] = jnp.concatenate([one, pad], axis=1)
        near_w[i, C:256] = jnp.zeros((64, C + L + 64), BF)
        far_w[i, 0:64] = jnp.zeros((64, C + L + 64), BF)
        far_w[i, 64:256] = jnp.concatenate([pad, one], axis=1)

    load_1.wait()

    def widen_1(i, carry):
        widen(i, wr1, near1, far1)
        return carry

    lax.fori_loop(0, 9, widen_1, 0)

    def recv_1(k, carry):
        i = lax.rem(s + NT - k, NT)
        pltpu.make_async_remote_copy(
            snd.at[0], got1.at[i], s1.at[k], r1.at[k], device_id={"space": i}
        ).wait_recv()
        return carry

    lax.fori_loop(1, NT, recv_1, 0)
    mine = chunk_of(s)
    strip = lax.div(mine, 8)
    side = jnp.where(strip == 0, 6, jnp.where(strip == 1, 1, jnp.where(strip == 2, 4, 3)))
    is_corner = (mine == 0) | (mine == 7) | (mine == 8) | (mine == 15)
    slot_of = lambda c: c + 1 + 2 * jnp.minimum(lax.div(c, 8), 1) + lax.div(c, 16)
    slot = slot_of(mine)
    corner = jnp.minimum(10 * strip + 9 * (1 - lax.div(lax.rem(mine, 8), 7)), 19)
    cside = jnp.where(mine == 0, 7, jnp.where(mine == 7, 5, jnp.where(mine == 8, 2, 0)))

    def pick(d, carry):
        snd2[0, d] = got1[nbr[side, d]]
        snd2[1, d] = got1[nbr[cside, d]]
        return carry

    lax.fori_loop(0, NT, pick, 0)

    def send_2(k):
        d = lax.rem(s + k, NT)
        return pltpu.make_async_remote_copy(
            snd2.at[0, d], got2.at[slot], s2.at[k], r2.at[k], device_id={"space": d}
        )

    def send_c(k):
        d = lax.rem(s + k, NT)
        return pltpu.make_async_remote_copy(
            snd2.at[1, d], got2.at[corner], sc.at[k], rc.at[corner], device_id={"space": d}
        )

    def start_2(i, carry):
        k = offset(i)
        send_2(k).start()

        @pl.when(is_corner)
        def _():
            send_c(k).start()

        return carry

    lax.fori_loop(0, NT - 1, start_2, 0)
    got2[slot] = snd2[0, s]

    @pl.when(is_corner)
    def _():
        got2[corner] = snd2[1, s]

    @pl.when(later)
    def _():
        t_act.wait_recv()

    def before(m, carry):
        for f in range(2):
            a = jnp.where(later, pact[m, f].astype(F32), 0.0)
            act[1, m + 1, f] = a.astype(BF)
            act[0, m + 1, f] = down(a, zero_row).astype(BF)
            act[2, m + 1, f] = up(a, zero_row).astype(BF)
        return carry

    lax.fori_loop(0, 8, before, 0)

    windows = []
    for p in range(3):
        for q in range(3):
            windows.append(
                jnp.concatenate(
                    [act[q, 1:8, p : p + 4].reshape(-1, L), act[q, 2:9, p : p + 4].reshape(-1, L)],
                    axis=1,
                )
            )
    acc[1:8] = conv_rows(windows, near1, far1).reshape(7, 4, 16, L)

    load_2.wait()

    def widen_2(i, carry):
        widen(i, wr2, near2, far2)
        return carry

    lax.fori_loop(0, 9, widen_2, 0)

    def recv_2(k, carry):
        i = lax.rem(s + NT - k, NT)
        pltpu.make_async_remote_copy(
            snd2.at[0, 0], got2.at[slot_of(chunk_of(i))], s2.at[k], r2.at[k], device_id={"space": i}
        ).wait_recv()
        return carry

    lax.fori_loop(1, NT, recv_2, 0)
    for place, c in ((9, 0), (0, 7), (19, 8), (10, 15)):

        @pl.when(mine != c)
        def _():
            pltpu.make_async_remote_copy(
                snd2.at[1, 0], got2.at[place], sc.at[0], rc.at[place],
                device_id={"space": device_of(c)},
            ).wait_recv()

    t_got = [
        to_next(2, got2.at[0:20], pgot.at[0:20]),
        to_next(3, got2.at[24:28], pgot.at[20:24]),
        to_next(4, got2.at[32:36], pgot.at[24:28]),
    ]

    @pl.when(sends)
    def _():
        for copy in t_got:
            copy.start()

    r8 = rows((8, L))
    upper = r8 < 4

    def keep(v):
        return jnp.where(later, v, 0.0)

    def wide(ref, i):
        return ref[i].astype(F32)

    def side_pair(m, f, pieces):
        a = jnp.concatenate(pieces, axis=0)
        act[1, m, f] = a.astype(BF)
        act[0, m, f] = down(a, zero_row).astype(BF)
        act[2, m, f] = up(a, zero_row).astype(BF)

    def side_pairs(ref, bases, first, count, into, clean):
        for m, base in zip((0, 9), bases):
            mixed = jnp.zeros((8, L), F32)
            for f in range(4 - count, 4):
                at = base + 2 * (f - 4 + count)
                pieces = [clean(wide(ref, at)), clean(wide(ref, at + 1))]
                side_pair(m, first + f - 4 + count, pieces)
                mixed = jnp.where(r8 == f, pieces[0][0:1], mixed)
                mixed = jnp.where(r8 == 4 + f, pieces[1][7:8], mixed)
            into[m] = mixed

    side_pairs(got2, (28, 20), 2, 4, inner, lambda v: v)
    for m in range(8):
        inner[m + 1] = jnp.where(upper, wide(snd, m), wide(snd, 8 + m))

    def two_frames(half, p, own, prev):
        if half == 1:
            return pltpu.roll(own, 8 - p, 0) if p else own
        if p == 2:
            return own
        if p == 0:
            return pltpu.roll(prev, 6, 0)
        return jnp.where(lax.rem(r8, 4) == 0, pltpu.roll(prev, 5, 0), pltpu.roll(own, 1, 0))

    duo = lax.div(r8, 2)
    none = jnp.zeros((8, L), F32)

    def ring_tiles(half, m):
        own = [wide(got2, 10 + m), wide(got2, m), inner[m]]
        prev = own
        if half == 0:
            prev = [keep(wide(pgot, 10 + m)), keep(wide(pgot, m)), pinner[m]]
        tiles = {}
        for p in range(3):
            t0, b0, o0 = [two_frames(half, p, a, b) for a, b in zip(own, prev)]
            b6 = pltpu.roll(b0, 6, 0)
            low = jnp.where(duo == 1, pltpu.roll(o0, 6, 0), jnp.where(duo == 3, none, t0))
            mid = jnp.where(duo == 0, pltpu.roll(t0, 4, 0), jnp.where(duo == 1, pltpu.roll(b0, 2, 0), none))
            top = jnp.where(duo == 0, o0, jnp.where(duo == 2, none, b6))
            for q, tile in enumerate((low, mid, top)):
                tiles[3 * p + q] = tile.astype(BF)
        return tiles

    for i in range(9):
        ring[1, i, 5, 8:16] = none.astype(BF)

    def rim(half):
        def pairs(u, carry):
            even, odd = ring_tiles(half, 2 * u), ring_tiles(half, 2 * u + 1)
            for i in range(9):
                ring[0, i, u + 1, 0:8] = even[i]
                ring[0, i, u + 1, 8:16] = odd[i]
                ring[1, i, u, 8:16] = even[i]
                ring[1, i, u + 1, 0:8] = odd[i]
            return carry

        lax.fori_loop(0, 5, pairs, 0)
        windows = []
        for p in range(3):
            for q in range(3):
                f = 2 * half + p
                sides = []
                for d in range(2):
                    sides.append(
                        jnp.concatenate(
                            [
                                act[q, d, f : f + 2].reshape(-1, L),
                                act[q, 8 + d, f : f + 2].reshape(-1, L),
                                ring[d, 3 * p + q, 1:6].reshape(-1, L),
                            ],
                            axis=0,
                        )
                    )
                windows.append(jnp.concatenate(sides, axis=1))
        total = conv_rows(windows, near1, far1)
        acc[0, 2 * half : 2 * half + 2] = total[0:32].reshape(2, 16, L)
        acc[8, 2 * half : 2 * half + 2] = total[32:64].reshape(2, 16, L)
        racc[...] = total[64:].reshape(10, 8, L)
        lax.fori_loop(0, 9, functools.partial(finish, half), 0)

    def finish(half, m, carry):
        rim_rows = racc[m]
        left_half = lanes((8, L)) < C

        def by_pair(left, middle, right):
            return jnp.where(m == 0, left, middle), jnp.where(m == 8, right, middle)

        t0, t1 = by_pair(near[0], near[1], near[2])
        u0, u1 = by_pair(near[5], near[6], near[7])
        o0, o1 = by_pair(near[3], own_valid, near[4])
        limit = jnp.where(r8 < 2, jnp.where(left_half, t0, t1), jnp.where(left_half, u0, u1))
        outer = norm_silu(rim_rows + bias1, gain2)
        outer = jnp.where(first_frame + 2 * half + lax.rem(r8, 2) < limit, outer, 0.0)
        if half == 1:
            hring[m] = outer.astype(BF)
        limit = jnp.where(lanes((16, L)) < C, o0, o1)
        r16 = rows((16, L))
        for g in range(2):
            f = 2 * half + g
            v = acc[m, f]
            v = v + jnp.where(r16 == 0, rim_rows[4 + g : 5 + g], 0.0)
            v = v + jnp.where(r16 == 15, rim_rows[6 + g : 7 + g], 0.0)
            h = norm_silu(v + bias1, gain2)
            h = jnp.where(first_frame + f < limit, h, 0.0)
            hid[1, m, f + 2] = h.astype(BF)
            hid[0, m, f + 2] = down(h, outer[g : g + 1]).astype(BF)
            hid[2, m, f + 2] = up(h, outer[2 + g : 3 + g]).astype(BF)
        return carry

    rim(1)
    t_hid = [to_next(5, hid.at[1, :, 4:6], phid), to_next(6, hring, phring)]

    @pl.when(sends)
    def _():
        for copy in t_hid:
            copy.start()

    @pl.when(later)
    def _():
        t_snd.wait_recv()
        for copy in t_got:
            copy.wait_recv()

    side_pairs(pgot, (24, 20), 0, 2, pinner, keep)
    for m in range(8):
        pinner[m + 1] = keep(jnp.where(upper, wide(psnd, m), wide(psnd, 8 + m)))
    rim(0)

    def conv2(half):
        windows = []
        for p in range(3):
            for q in range(3):
                f = 2 * half + p
                windows.append(
                    jnp.concatenate(
                        [hid[q, 0:8, f : f + 2].reshape(-1, L), hid[q, 1:9, f : f + 2].reshape(-1, L)],
                        axis=1,
                    )
                )
        total = conv_rows(windows, near2, far2)
        total = total.reshape(8, 2, 16, L)
        for g in range(2):
            f = 2 * half + g
            there = first_frame + f < own_valid
            for m in range(8):
                x = vid[f, :, L * m : L * m + L].astype(F32)
                o = jnp.where(there, total[m, g] + bias2 + x, 0.0)
                out[f, 0, :, L * m : L * m + L] = o.astype(BF)

    conv2(1)

    @pl.when(later)
    def _():
        for copy in t_hid:
            copy.wait_recv()

    def before_2(m, carry):
        rim_rows = keep(phring[m].astype(F32))
        for f in range(2):
            h = keep(phid[m, f].astype(F32))
            hid[1, m, f] = h.astype(BF)
            hid[0, m, f] = down(h, rim_rows[f : f + 1]).astype(BF)
            hid[2, m, f] = up(h, rim_rows[2 + f : 3 + f]).astype(BF)
        return carry

    lax.fori_loop(0, 9, before_2, 0)
    conv2(0)

    def sent(k, carry):
        send_1(k).wait_send()
        send_2(k).wait_send()
        return carry

    lax.fori_loop(1, NT, sent, 0)

    @pl.when(is_corner)
    def _():
        def sent_c(k, carry):
            send_c(k).wait_send()
            return carry

        lax.fori_loop(1, NT, sent_c, 0)

    @pl.when(sends)
    def _():
        for copy in [t_act, t_snd, *t_got, *t_hid]:
            copy.wait_send()


def on_device(video, nbr, vf, g1, w1, b1, g2, w2, b2):
    vmem = lambda *shape, dtype=BF: pltpu.VMEM(shape, dtype)
    dma = lambda n: pltpu.SemaphoreType.DMA((n,))
    hbm = pl.BlockSpec(memory_space=pltpu.HBM)
    local = pl.BlockSpec(memory_space=pltpu.VMEM)
    return pl.pallas_call(
        kernel,
        out_shape=pltpu.VMEM(video.shape, BF),
        in_specs=[hbm] * 9,
        out_specs=local,
        scratch_shapes=[
            pltpu.SMEM((8, NT), jnp.int32),
            pltpu.SMEM((NT,), jnp.int32),
            *[vmem(C, dtype=F32)] * 4,
            vmem(4, 16, 16 * C),
            vmem(9, C, 3 * C),
            vmem(9, C, 3 * C),
            *[vmem(9, 256, C + L + 64)] * 4,
            vmem(3, 10, 6, 16, L),
            vmem(16, 8, L, dtype=F32),
            vmem(32, 8, L),
            vmem(NT + 1, 8, L),
            vmem(2, NT, 8, L),
            vmem(36, 8, L),
            vmem(8, 2, 16, L),
            vmem(16, 8, L),
            vmem(28, 8, L),
            vmem(10, 8, L, dtype=F32),
            vmem(10, 8, L, dtype=F32),
            vmem(2, 9, 6, 16, L),
            vmem(9, 4, 16, L, dtype=F32),
            vmem(10, 8, L, dtype=F32),
            vmem(3, 9, 6, 16, L),
            vmem(9, 8, L),
            vmem(9, 2, 16, L),
            vmem(9, 8, L),
            dma(9), dma(NT), dma(NT), dma(NT), dma(NT), dma(NT), dma(20), dma(7), dma(7),
        ],
        compiler_params=pltpu.CompilerParams(
            collective_id=0, has_side_effects=True, vmem_limit_bytes=66000000
        ),
    )(video, nbr.T, vf, g1, jnp.swapaxes(w1, 1, 2), b1, g2, jnp.swapaxes(w2, 1, 2), b2)


def solution(mesh):
    placed = (P("tm", "space", None, None), P(), P(), P(), P(), P(), P(), P(), P())
    return jax.shard_map(
        on_device, mesh=mesh, in_specs=placed, out_specs=P("tm", "space", None, None), check_vma=False
    )
```

```python
import functools

import jax
import jax.numpy as jnp
from jax import lax
from jax.experimental import pallas as pl
from jax.experimental.pallas import tpu as pltpu
from jax.sharding import PartitionSpec as P

EPS = 1e-06
BF = jnp.bfloat16
F32 = jnp.float32
NT = 32
TM = 8
C = 192
L = 2 * C


def chunk_of(dev):
    z, y = lax.div(dev, 4), lax.rem(dev, 4)
    strip = lax.rem(y, 2) * 2 + lax.div(y, 2)
    return strip * 8 + lax.rem(3 * (z + 16 - 2 * strip), 8)


def device_of(chunk):
    strip, low = chunk // 8, chunk % 8
    return ((3 * low + 2 * strip) % 8) * 4 + (strip % 2) * 2 + strip // 2


def offset(i):
    return 16 + (1 - 2 * lax.rem(i, 2)) * lax.div(i + 1, 2)


def lanes(shape):
    return lax.broadcasted_iota(jnp.int32, shape, len(shape) - 1)


def rows(shape):
    return lax.broadcasted_iota(jnp.int32, shape, len(shape) - 2)


def norm_silu(v, gain):
    sq = v * v
    low = lanes((v.shape[0], 128)) < 64
    mid = sq[:, 128:256]
    zero = jnp.zeros_like(mid)
    first = jnp.sum(sq[:, :128] + jnp.where(low, mid, zero), axis=-1, keepdims=True)
    second = jnp.sum(sq[:, 256:] + jnp.where(low, zero, mid), axis=-1, keepdims=True)
    first = lax.rsqrt(first * (1.0 / C) + EPS)
    second = lax.rsqrt(second * (1.0 / C) + EPS)
    y = v * jnp.where(lanes(v.shape) < C, first, second) * gain
    half = 0.5 * y
    return half + half * jnp.tanh(half)


def matmul(a, b):
    return jnp.dot(a, b, preferred_element_type=F32)


def conv_rows(windows, near_w, far_w):
    first = jnp.concatenate([w[:, : C + L + 64] for w in windows], axis=1)
    second = jnp.concatenate([w[:, 128:] for w in windows], axis=1)
    near_w = near_w[...].reshape(-1, 256)
    far_w = far_w[...].reshape(-1, 256)
    a, b = matmul(first, near_w), matmul(second, far_w)
    return jnp.concatenate([a[:, :128], a[:, 128:] + b[:, :128], b[:, 128:]], axis=1)


def down(v, first_row):
    return jnp.where(rows(v.shape) == 0, first_row, pltpu.roll(v, 1, 0))


def up(v, last_row):
    n = v.shape[0]
    return jnp.where(rows(v.shape) == n - 1, last_row, pltpu.roll(v, n - 1, 0))


def kernel(
    video, nbr_in, vf_in, g1_in, w1, b1_in, g2_in, w2, b2_in, out,
    nbr, vf, g1, b1, g2, b2, vid, wr1, wr2, near1, far1, near2, far2, act, strip32, snd, got1, snd2, got2,
    pact, psnd, pgot, inner, pinner, ring, acc, racc, hid, hring, phid, phring,
    lsem, s1, r1, s2, r2, sc, rc, st, rt,
):
    t, s = lax.axis_index("tm"), lax.axis_index("space")
    nxt, prv = lax.rem(t + 1, TM), lax.rem(t + TM - 1, TM)

    barrier = pltpu.get_barrier_semaphore()

    later, sends = t > 0, t < TM - 1

    def greet(i, carry):
        pl.semaphore_signal(barrier, inc=1, device_id={"space": lax.rem(s + offset(i), NT)})
        return carry

    lax.fori_loop(0, NT - 1, greet, 0)

    @pl.when(sends)
    def _():
        pl.semaphore_signal(barrier, inc=1, device_id={"tm": nxt})

    @pl.when(later)
    def _():
        pl.semaphore_signal(barrier, inc=1, device_id={"tm": prv})

    loads = [
        pltpu.make_async_copy(src, dst, lsem.at[3 + i])
        for i, (src, dst) in enumerate(
            ((nbr_in, nbr), (vf_in, vf), (g1_in, g1), (b1_in, b1), (g2_in, g2), (b2_in, b2))
        )
    ]
    for copy in loads:
        copy.start()
    load_v = pltpu.make_async_copy(video.at[:, 0], vid, lsem.at[0])
    load_v.start()
    load_1 = pltpu.make_async_copy(w1, wr1, lsem.at[1])
    load_1.start()
    load_2 = pltpu.make_async_copy(w2, wr2, lsem.at[2])
    load_2.start()

    for copy in loads:
        copy.wait()

    def twice(ref):
        one = ref[...].reshape(1, C)
        return jnp.concatenate([one, one], axis=1)

    gain1, bias1, gain2, bias2 = twice(g1), twice(b1), twice(g2), twice(b2)
    first_frame = 4 * t
    own_valid = vf[s]

    def valid_of(k):
        n = nbr[k, s]
        return jnp.where(n < NT, vf[jnp.minimum(n, NT - 1)], 0)

    near = [valid_of(k) for k in range(8)]
    zero_row = jnp.zeros((1, L), F32)

    load_v.wait()
    for f in range(4):
        there = first_frame + f < own_valid
        for m in range(8):
            a = norm_silu(vid[f, :, L * m : L * m + L].astype(F32), gain1)
            a = jnp.where(there, a, 0.0)
            act[1, m + 1, f + 2] = a.astype(BF)
            act[0, m + 1, f + 2] = down(a, zero_row).astype(BF)
            act[2, m + 1, f + 2] = up(a, zero_row).astype(BF)
            strip32[m, f : f + 1] = a[0:1]
            strip32[m, 4 + f : 5 + f] = a[1:2]
            strip32[8 + m, f : f + 1] = a[14:15]
            strip32[8 + m, 4 + f : 5 + f] = a[15:16]
            if m in (0, 7):
                base = (16 if m == 0 else 24) + 2 * f
                snd[base] = a[0:8].astype(BF)
                snd[base + 1] = a[8:16].astype(BF)
    for c in range(16):
        snd[c] = strip32[c].astype(BF)
    got1[NT] = jnp.zeros((8, L), BF)

    def widen(i, raw, near_w, far_w):
        one, pad = raw[i], jnp.zeros((64, 3 * C), BF)
        near_w[i, 0 : 3 * C] = jnp.concatenate([one, pad], axis=0).T
        near_w[i, 3 * C : 3 * C + 64] = jnp.zeros((64, 256), BF)
        far_w[i, 0:64] = jnp.zeros((64, 256), BF)
        far_w[i, 64 : 64 + 3 * C] = jnp.concatenate([pad, one], axis=0).T


    pl.semaphore_wait(barrier, NT - 1 + jnp.where(later, 1, 0) + jnp.where(sends, 1, 0))

    def send_1(k):
        j = lax.rem(s + k, NT)
        return pltpu.make_async_remote_copy(
            snd.at[chunk_of(j)], got1.at[s], s1.at[k], r1.at[k], device_id={"space": j}
        )

    def start_1(i, carry):
        send_1(offset(i)).start()
        return carry

    lax.fori_loop(0, NT - 1, start_1, 0)
    got1[s] = snd[chunk_of(s)]

    def to_next(i, src, dst):
        return pltpu.make_async_remote_copy(src, dst, st.at[i], rt.at[i], device_id={"tm": nxt})

    t_act = to_next(0, act.at[1, 1:9, 4:6], pact)
    t_snd = to_next(1, snd.at[0:16], psnd)

    @pl.when(sends)
    def _():
        t_act.start()
        t_snd.start()

    load_1.wait()

    def widen_1(i, carry):
        widen(i, wr1, near1, far1)
        return carry

    lax.fori_loop(0, 9, widen_1, 0)
    load_2.wait()

    def widen_2(i, carry):
        widen(i, wr2, near2, far2)
        return carry

    lax.fori_loop(0, 9, widen_2, 0)

    def recv_1(k, carry):
        i = lax.rem(s + NT - k, NT)
        pltpu.make_async_remote_copy(
            snd.at[0], got1.at[i], s1.at[k], r1.at[k], device_id={"space": i}
        ).wait_recv()
        return carry

    lax.fori_loop(1, NT, recv_1, 0)
    mine = chunk_of(s)
    strip = lax.div(mine, 8)
    side = jnp.where(strip == 0, 6, jnp.where(strip == 1, 1, jnp.where(strip == 2, 4, 3)))
    is_corner = (mine == 0) | (mine == 7) | (mine == 8) | (mine == 15)
    slot_of = lambda c: c + 1 + 2 * jnp.minimum(lax.div(c, 8), 1) + lax.div(c, 16)
    slot = slot_of(mine)
    corner = jnp.minimum(10 * strip + 9 * (1 - lax.div(lax.rem(mine, 8), 7)), 19)
    cside = jnp.where(mine == 0, 7, jnp.where(mine == 7, 5, jnp.where(mine == 8, 2, 0)))

    def pick(d, carry):
        snd2[0, d] = got1[nbr[side, d]]
        snd2[1, d] = got1[nbr[cside, d]]
        return carry

    lax.fori_loop(0, NT, pick, 0)

    def send_2(k):
        d = lax.rem(s + k, NT)
        return pltpu.make_async_remote_copy(
            snd2.at[0, d], got2.at[slot], s2.at[k], r2.at[k], device_id={"space": d}
        )

    def send_c(k):
        d = lax.rem(s + k, NT)
        return pltpu.make_async_remote_copy(
            snd2.at[1, d], got2.at[corner], sc.at[k], rc.at[corner], device_id={"space": d}
        )

    def start_2(i, carry):
        k = offset(i)
        send_2(k).start()

        @pl.when(is_corner)
        def _():
            send_c(k).start()

        return carry

    lax.fori_loop(0, NT - 1, start_2, 0)
    got2[slot] = snd2[0, s]

    @pl.when(is_corner)
    def _():
        got2[corner] = snd2[1, s]

    @pl.when(later)
    def _():
        t_act.wait_recv()

    def before(m, carry):
        for f in range(2):
            a = jnp.where(later, pact[m, f].astype(F32), 0.0)
            act[1, m + 1, f] = a.astype(BF)
            act[0, m + 1, f] = down(a, zero_row).astype(BF)
            act[2, m + 1, f] = up(a, zero_row).astype(BF)
        return carry

    lax.fori_loop(0, 8, before, 0)

    windows = []
    for p in range(3):
        for q in range(3):
            windows.append(
                jnp.concatenate(
                    [act[q, 1:8, p : p + 4].reshape(-1, L), act[q, 2:9, p : p + 4].reshape(-1, L)],
                    axis=1,
                )
            )
    acc[1:8] = conv_rows(windows, near1, far1).reshape(7, 4, 16, L)

    def recv_2(k, carry):
        i = lax.rem(s + NT - k, NT)
        pltpu.make_async_remote_copy(
            snd2.at[0, 0], got2.at[slot_of(chunk_of(i))], s2.at[k], r2.at[k], device_id={"space": i}
        ).wait_recv()
        return carry

    lax.fori_loop(1, NT, recv_2, 0)
    for place, c in ((9, 0), (0, 7), (19, 8), (10, 15)):

        @pl.when(mine != c)
        def _():
            pltpu.make_async_remote_copy(
                snd2.at[1, 0], got2.at[place], sc.at[0], rc.at[place],
                device_id={"space": device_of(c)},
            ).wait_recv()

    t_got = [
        to_next(2, got2.at[0:20], pgot.at[0:20]),
        to_next(3, got2.at[24:28], pgot.at[20:24]),
        to_next(4, got2.at[32:36], pgot.at[24:28]),
    ]

    @pl.when(sends)
    def _():
        for copy in t_got:
            copy.start()

    r8 = rows((8, L))
    upper = r8 < 4

    def keep(v):
        return jnp.where(later, v, 0.0)

    def wide(ref, i):
        return ref[i].astype(F32)

    def side_pair(m, f, pieces):
        a = jnp.concatenate(pieces, axis=0)
        act[1, m, f] = a.astype(BF)
        act[0, m, f] = down(a, zero_row).astype(BF)
        act[2, m, f] = up(a, zero_row).astype(BF)

    def side_pairs(ref, bases, first, count, into, clean):
        for m, base in zip((0, 9), bases):
            mixed = jnp.zeros((8, L), F32)
            for f in range(4 - count, 4):
                at = base + 2 * (f - 4 + count)
                pieces = [clean(wide(ref, at)), clean(wide(ref, at + 1))]
                side_pair(m, first + f - 4 + count, pieces)
                mixed = jnp.where(r8 == f, pieces[0][0:1], mixed)
                mixed = jnp.where(r8 == 4 + f, pieces[1][7:8], mixed)
            into[m] = mixed

    side_pairs(got2, (28, 20), 2, 4, inner, lambda v: v)
    for m in range(8):
        inner[m + 1] = jnp.where(upper, wide(snd, m), wide(snd, 8 + m))

    def two_frames(half, p, own, prev):
        if half == 1:
            return pltpu.roll(own, 8 - p, 0) if p else own
        if p == 2:
            return own
        if p == 0:
            return pltpu.roll(prev, 6, 0)
        return jnp.where(lax.rem(r8, 4) == 0, pltpu.roll(prev, 5, 0), pltpu.roll(own, 1, 0))

    duo = lax.div(r8, 2)
    none = jnp.zeros((8, L), F32)

    def ring_tiles(half, m):
        own = [wide(got2, 10 + m), wide(got2, m), inner[m]]
        prev = own
        if half == 0:
            prev = [keep(wide(pgot, 10 + m)), keep(wide(pgot, m)), pinner[m]]
        tiles = {}
        for p in range(3):
            t0, b0, o0 = [two_frames(half, p, a, b) for a, b in zip(own, prev)]
            b6 = pltpu.roll(b0, 6, 0)
            low = jnp.where(duo == 1, pltpu.roll(o0, 6, 0), jnp.where(duo == 3, none, t0))
            mid = jnp.where(duo == 0, pltpu.roll(t0, 4, 0), jnp.where(duo == 1, pltpu.roll(b0, 2, 0), none))
            top = jnp.where(duo == 0, o0, jnp.where(duo == 2, none, b6))
            for q, tile in enumerate((low, mid, top)):
                tiles[3 * p + q] = tile.astype(BF)
        return tiles

    for i in range(9):
        ring[1, i, 5, 8:16] = none.astype(BF)

    def rim(half):
        def pairs(u, carry):
            even, odd = ring_tiles(half, 2 * u), ring_tiles(half, 2 * u + 1)
            for i in range(9):
                ring[0, i, u + 1, 0:8] = even[i]
                ring[0, i, u + 1, 8:16] = odd[i]
                ring[1, i, u, 8:16] = even[i]
                ring[1, i, u + 1, 0:8] = odd[i]
            return carry

        lax.fori_loop(0, 5, pairs, 0)
        windows = []
        for p in range(3):
            for q in range(3):
                f = 2 * half + p
                sides = []
                for d in range(2):
                    sides.append(
                        jnp.concatenate(
                            [
                                act[q, d, f : f + 2].reshape(-1, L),
                                act[q, 8 + d, f : f + 2].reshape(-1, L),
                                ring[d, 3 * p + q, 1:6].reshape(-1, L),
                            ],
                            axis=0,
                        )
                    )
                windows.append(jnp.concatenate(sides, axis=1))
        total = conv_rows(windows, near1, far1)
        acc[0, 2 * half : 2 * half + 2] = total[0:32].reshape(2, 16, L)
        acc[8, 2 * half : 2 * half + 2] = total[32:64].reshape(2, 16, L)
        racc[...] = total[64:].reshape(10, 8, L)
        lax.fori_loop(0, 9, functools.partial(finish, half), 0)

    def finish(half, m, carry):
        rim_rows = racc[m]
        left_half = lanes((8, L)) < C

        def by_pair(left, middle, right):
            return jnp.where(m == 0, left, middle), jnp.where(m == 8, right, middle)

        t0, t1 = by_pair(near[0], near[1], near[2])
        u0, u1 = by_pair(near[5], near[6], near[7])
        o0, o1 = by_pair(near[3], own_valid, near[4])
        limit = jnp.where(r8 < 2, jnp.where(left_half, t0, t1), jnp.where(left_half, u0, u1))
        outer = norm_silu(rim_rows + bias1, gain2)
        outer = jnp.where(first_frame + 2 * half + lax.rem(r8, 2) < limit, outer, 0.0)
        if half == 1:
            hring[m] = outer.astype(BF)
        limit = jnp.where(lanes((16, L)) < C, o0, o1)
        r16 = rows((16, L))
        for g in range(2):
            f = 2 * half + g
            v = acc[m, f]
            v = v + jnp.where(r16 == 0, rim_rows[4 + g : 5 + g], 0.0)
            v = v + jnp.where(r16 == 15, rim_rows[6 + g : 7 + g], 0.0)
            h = norm_silu(v + bias1, gain2)
            h = jnp.where(first_frame + f < limit, h, 0.0)
            hid[1, m, f + 2] = h.astype(BF)
            hid[0, m, f + 2] = down(h, outer[g : g + 1]).astype(BF)
            hid[2, m, f + 2] = up(h, outer[2 + g : 3 + g]).astype(BF)
        return carry

    rim(1)
    t_hid = [to_next(5, hid.at[1, :, 4:6], phid), to_next(6, hring, phring)]

    @pl.when(sends)
    def _():
        for copy in t_hid:
            copy.start()

    @pl.when(later)
    def _():
        t_snd.wait_recv()
        for copy in t_got:
            copy.wait_recv()

    side_pairs(pgot, (24, 20), 0, 2, pinner, keep)
    for m in range(8):
        pinner[m + 1] = keep(jnp.where(upper, wide(psnd, m), wide(psnd, 8 + m)))
    rim(0)

    def conv2(half):
        windows = []
        for p in range(3):
            for q in range(3):
                f = 2 * half + p
                windows.append(
                    jnp.concatenate(
                        [hid[q, 0:8, f : f + 2].reshape(-1, L), hid[q, 1:9, f : f + 2].reshape(-1, L)],
                        axis=1,
                    )
                )
        total = conv_rows(windows, near2, far2)
        total = total.reshape(8, 2, 16, L)
        for g in range(2):
            f = 2 * half + g
            there = first_frame + f < own_valid
            for m in range(8):
                x = vid[f, :, L * m : L * m + L].astype(F32)
                o = jnp.where(there, total[m, g] + bias2 + x, 0.0)
                out[f, 0, :, L * m : L * m + L] = o.astype(BF)

    conv2(1)

    @pl.when(later)
    def _():
        for copy in t_hid:
            copy.wait_recv()

    def before_2(m, carry):
        rim_rows = keep(phring[m].astype(F32))
        for f in range(2):
            h = keep(phid[m, f].astype(F32))
            hid[1, m, f] = h.astype(BF)
            hid[0, m, f] = down(h, rim_rows[f : f + 1]).astype(BF)
            hid[2, m, f] = up(h, rim_rows[2 + f : 3 + f]).astype(BF)
        return carry

    lax.fori_loop(0, 9, before_2, 0)
    conv2(0)

    def sent(k, carry):
        send_1(k).wait_send()
        send_2(k).wait_send()
        return carry

    lax.fori_loop(1, NT, sent, 0)

    @pl.when(is_corner)
    def _():
        def sent_c(k, carry):
            send_c(k).wait_send()
            return carry

        lax.fori_loop(1, NT, sent_c, 0)

    @pl.when(sends)
    def _():
        for copy in [t_act, t_snd, *t_got, *t_hid]:
            copy.wait_send()


def on_device(video, nbr, vf, g1, w1, b1, g2, w2, b2):
    vmem = lambda *shape, dtype=BF: pltpu.VMEM(shape, dtype)
    dma = lambda n: pltpu.SemaphoreType.DMA((n,))
    hbm = pl.BlockSpec(memory_space=pltpu.HBM)
    local = pl.BlockSpec(memory_space=pltpu.VMEM)
    return pl.pallas_call(
        kernel,
        out_shape=pltpu.VMEM(video.shape, BF),
        in_specs=[hbm] * 9,
        out_specs=local,
        scratch_shapes=[
            pltpu.SMEM((8, NT), jnp.int32),
            pltpu.SMEM((NT,), jnp.int32),
            *[vmem(C, dtype=F32)] * 4,
            vmem(4, 16, 16 * C),
            vmem(9, C, 3 * C),
            vmem(9, C, 3 * C),
            *[vmem(9, C + L + 64, 256)] * 4,
            vmem(3, 10, 6, 16, L),
            vmem(16, 8, L, dtype=F32),
            vmem(32, 8, L),
            vmem(NT + 1, 8, L),
            vmem(2, NT, 8, L),
            vmem(36, 8, L),
            vmem(8, 2, 16, L),
            vmem(16, 8, L),
            vmem(28, 8, L),
            vmem(10, 8, L, dtype=F32),
            vmem(10, 8, L, dtype=F32),
            vmem(2, 9, 6, 16, L),
            vmem(9, 4, 16, L, dtype=F32),
            vmem(10, 8, L, dtype=F32),
            vmem(3, 9, 6, 16, L),
            vmem(9, 8, L),
            vmem(9, 2, 16, L),
            vmem(9, 8, L),
            dma(9), dma(NT), dma(NT), dma(NT), dma(NT), dma(NT), dma(20), dma(7), dma(7),
        ],
        compiler_params=pltpu.CompilerParams(
            collective_id=0, has_side_effects=True, vmem_limit_bytes=66000000
        ),
    )(video, nbr.T, vf, g1, jnp.swapaxes(w1, 1, 2), b1, g2, jnp.swapaxes(w2, 1, 2), b2)


def solution(mesh):
    placed = (P("tm", "space", None, None), P(), P(), P(), P(), P(), P(), P(), P())
    return jax.shard_map(
        on_device, mesh=mesh, in_specs=placed, out_specs=P("tm", "space", None, None), check_vma=False
    )
```

```python
import functools

import jax
import jax.numpy as jnp
from jax import lax
from jax.experimental import pallas as pl
from jax.experimental.pallas import tpu as pltpu
from jax.sharding import PartitionSpec as P

EPS = 1e-06
BF = jnp.bfloat16
F32 = jnp.float32
NT = 32
TM = 8
C = 192
L = 2 * C


def chunk_of(dev):
    odd = lax.rem(lax.axis_index("tm"), 2)
    z, y = lax.div(dev, 4), lax.rem(dev, 4)
    y = y + odd * (1 - 2 * lax.rem(y, 2))
    strip = lax.rem(y, 2) * 2 + lax.div(y, 2)
    return strip * 8 + lax.rem(3 * (z + 16 - 2 * strip), 8)


def device_of(chunk):
    odd = lax.rem(lax.axis_index("tm"), 2)
    strip, low = chunk // 8, chunk % 8
    y = (strip % 2) * 2 + strip // 2
    return ((3 * low + 2 * strip) % 8) * 4 + y + odd * (1 - 2 * (y % 2))


def offset(i):
    return 16 + (1 - 2 * lax.rem(i, 2)) * lax.div(i + 1, 2)


def lanes(shape):
    return lax.broadcasted_iota(jnp.int32, shape, len(shape) - 1)


def rows(shape):
    return lax.broadcasted_iota(jnp.int32, shape, len(shape) - 2)


def norm_silu(v, gain):
    sq = v * v
    low = lanes((v.shape[0], 128)) < 64
    mid = sq[:, 128:256]
    zero = jnp.zeros_like(mid)
    first = jnp.sum(sq[:, :128] + jnp.where(low, mid, zero), axis=-1, keepdims=True)
    second = jnp.sum(sq[:, 256:] + jnp.where(low, zero, mid), axis=-1, keepdims=True)
    first = lax.rsqrt(first * (1.0 / C) + EPS)
    second = lax.rsqrt(second * (1.0 / C) + EPS)
    y = v * jnp.where(lanes(v.shape) < C, first, second) * gain
    half = 0.5 * y
    return half + half * jnp.tanh(half)


def matmul(a, b):
    return jnp.dot(a, b, preferred_element_type=F32)


def conv_rows(windows, near_w, far_w):
    first = jnp.concatenate([w[:, : C + L + 64] for w in windows], axis=1)
    second = jnp.concatenate([w[:, 128:] for w in windows], axis=1)
    near_w = near_w[...].reshape(-1, 256)
    far_w = far_w[...].reshape(-1, 256)
    a, b = matmul(first, near_w), matmul(second, far_w)
    return jnp.concatenate([a[:, :128], a[:, 128:] + b[:, :128], b[:, 128:]], axis=1)


def down(v, first_row):
    return jnp.where(rows(v.shape) == 0, first_row, pltpu.roll(v, 1, 0))


def up(v, last_row):
    n = v.shape[0]
    return jnp.where(rows(v.shape) == n - 1, last_row, pltpu.roll(v, n - 1, 0))


def kernel(
    video, nbr_in, vf_in, g1_in, w1, b1_in, g2_in, w2, b2_in, out,
    nbr, vf, g1, b1, g2, b2, vid, wr1, wr2, near1, far1, near2, far2, act, strip32, snd, got1, snd2, got2,
    pact, psnd, pgot, inner, pinner, ring, acc, racc, hid, hring, phid, phring,
    lsem, s1, r1, s2, r2, sc, rc, st, rt,
):
    t, s = lax.axis_index("tm"), lax.axis_index("space")
    nxt, prv = lax.rem(t + 1, TM), lax.rem(t + TM - 1, TM)

    barrier = pltpu.get_barrier_semaphore()

    later, sends = t > 0, t < TM - 1

    def greet(i, carry):
        pl.semaphore_signal(barrier, inc=1, device_id={"space": lax.rem(s + offset(i), NT)})
        return carry

    lax.fori_loop(0, NT - 1, greet, 0, unroll=True)

    @pl.when(sends)
    def _():
        pl.semaphore_signal(barrier, inc=1, device_id={"tm": nxt})

    @pl.when(later)
    def _():
        pl.semaphore_signal(barrier, inc=1, device_id={"tm": prv})

    loads = [
        pltpu.make_async_copy(src, dst, lsem.at[3 + i])
        for i, (src, dst) in enumerate(
            ((nbr_in, nbr), (vf_in, vf), (g1_in, g1), (b1_in, b1), (g2_in, g2), (b2_in, b2))
        )
    ]
    for copy in loads:
        copy.start()
    load_v = pltpu.make_async_copy(video.at[:, 0], vid, lsem.at[0])
    load_v.start()
    load_1 = pltpu.make_async_copy(w1, wr1, lsem.at[1])
    load_1.start()
    load_2 = pltpu.make_async_copy(w2, wr2, lsem.at[2])
    load_2.start()

    for copy in loads:
        copy.wait()

    def twice(ref):
        one = ref[...].reshape(1, C)
        return jnp.concatenate([one, one], axis=1)

    gain1, bias1, gain2, bias2 = twice(g1), twice(b1), twice(g2), twice(b2)
    first_frame = 4 * t
    own_valid = vf[s]

    def valid_of(k):
        n = nbr[k, s]
        return jnp.where(n < NT, vf[jnp.minimum(n, NT - 1)], 0)

    near = [valid_of(k) for k in range(8)]
    zero_row = jnp.zeros((1, L), F32)

    load_v.wait()
    for f in range(4):
        there = first_frame + f < own_valid
        for m in range(8):
            a = norm_silu(vid[f, :, L * m : L * m + L].astype(F32), gain1)
            a = jnp.where(there, a, 0.0)
            act[1, m + 1, f + 2] = a.astype(BF)
            act[0, m + 1, f + 2] = down(a, zero_row).astype(BF)
            act[2, m + 1, f + 2] = up(a, zero_row).astype(BF)
            strip32[m, f : f + 1] = a[0:1]
            strip32[m, 4 + f : 5 + f] = a[1:2]
            strip32[8 + m, f : f + 1] = a[14:15]
            strip32[8 + m, 4 + f : 5 + f] = a[15:16]
            if m in (0, 7):
                base = (16 if m == 0 else 24) + 2 * f
                snd[base] = a[0:8].astype(BF)
                snd[base + 1] = a[8:16].astype(BF)
    for c in range(16):
        snd[c] = strip32[c].astype(BF)
    got1[NT] = jnp.zeros((8, L), BF)

    def widen(i, raw, near_w, far_w):
        one, pad = raw[i], jnp.zeros((64, 3 * C), BF)
        near_w[i, 0 : 3 * C] = jnp.concatenate([one, pad], axis=0).T
        near_w[i, 3 * C : 3 * C + 64] = jnp.zeros((64, 256), BF)
        far_w[i, 0:64] = jnp.zeros((64, 256), BF)
        far_w[i, 64 : 64 + 3 * C] = jnp.concatenate([pad, one], axis=0).T


    pl.semaphore_wait(barrier, NT - 1 + jnp.where(later, 1, 0) + jnp.where(sends, 1, 0))

    def send_1(k):
        j = lax.rem(s + k, NT)
        return pltpu.make_async_remote_copy(
            snd.at[chunk_of(j)], got1.at[s], s1.at[k], r1.at[k], device_id={"space": j}
        )

    def start_1(i, carry):
        send_1(offset(i)).start()
        return carry

    lax.fori_loop(0, NT - 1, start_1, 0)
    got1[s] = snd[chunk_of(s)]

    def to_next(i, src, dst):
        return pltpu.make_async_remote_copy(src, dst, st.at[i], rt.at[i], device_id={"tm": nxt})

    t_act = to_next(0, act.at[1, 1:9, 4:6], pact)
    t_snd = to_next(1, snd.at[0:16], psnd)

    @pl.when(sends)
    def _():
        t_act.start()
        t_snd.start()

    load_1.wait()

    def widen_1(i, carry):
        widen(i, wr1, near1, far1)
        return carry

    lax.fori_loop(0, 9, widen_1, 0)
    load_2.wait()

    def widen_2(i, carry):
        widen(i, wr2, near2, far2)
        return carry

    lax.fori_loop(0, 9, widen_2, 0)

    def recv_1(k, carry):
        i = lax.rem(s + NT - k, NT)
        pltpu.make_async_remote_copy(
            snd.at[0], got1.at[i], s1.at[k], r1.at[k], device_id={"space": i}
        ).wait_recv()
        return carry

    lax.fori_loop(1, NT, recv_1, 0)
    mine = chunk_of(s)
    strip = lax.div(mine, 8)
    side = jnp.where(strip == 0, 6, jnp.where(strip == 1, 1, jnp.where(strip == 2, 4, 3)))
    is_corner = (mine == 0) | (mine == 7) | (mine == 8) | (mine == 15)
    slot_of = lambda c: c + 1 + 2 * jnp.minimum(lax.div(c, 8), 1) + lax.div(c, 16)
    slot = slot_of(mine)
    corner = jnp.minimum(10 * strip + 9 * (1 - lax.div(lax.rem(mine, 8), 7)), 19)
    cside = jnp.where(mine == 0, 7, jnp.where(mine == 7, 5, jnp.where(mine == 8, 2, 0)))

    def pick(d, carry):
        snd2[0, d] = got1[nbr[side, d]]
        snd2[1, d] = got1[nbr[cside, d]]
        return carry

    lax.fori_loop(0, NT, pick, 0, unroll=True)

    def send_2(k):
        d = lax.rem(s + k, NT)
        return pltpu.make_async_remote_copy(
            snd2.at[0, d], got2.at[slot], s2.at[k], r2.at[k], device_id={"space": d}
        )

    def send_c(k):
        d = lax.rem(s + k, NT)
        return pltpu.make_async_remote_copy(
            snd2.at[1, d], got2.at[corner], sc.at[k], rc.at[corner], device_id={"space": d}
        )

    def start_2(i, carry):
        k = offset(i)
        send_2(k).start()

        @pl.when(is_corner)
        def _():
            send_c(k).start()

        return carry

    lax.fori_loop(0, NT - 1, start_2, 0)
    got2[slot] = snd2[0, s]

    @pl.when(is_corner)
    def _():
        got2[corner] = snd2[1, s]

    @pl.when(later)
    def _():
        t_act.wait_recv()

    def before(m, carry):
        for f in range(2):
            a = jnp.where(later, pact[m, f].astype(F32), 0.0)
            act[1, m + 1, f] = a.astype(BF)
            act[0, m + 1, f] = down(a, zero_row).astype(BF)
            act[2, m + 1, f] = up(a, zero_row).astype(BF)
        return carry

    lax.fori_loop(0, 8, before, 0)

    windows = []
    for p in range(3):
        for q in range(3):
            windows.append(
                jnp.concatenate(
                    [act[q, 1:8, p : p + 4].reshape(-1, L), act[q, 2:9, p : p + 4].reshape(-1, L)],
                    axis=1,
                )
            )
    acc[1:8] = conv_rows(windows, near1, far1).reshape(7, 4, 16, L)

    def early(m, carry):
        for f in range(4):
            h = norm_silu(acc[m, f] + bias1, gain2)
            h = jnp.where(first_frame + f < own_valid, h, 0.0)
            hid[1, m, f + 2] = h.astype(BF)
            hid[0, m, f + 2] = down(h, zero_row).astype(BF)
            hid[2, m, f + 2] = up(h, zero_row).astype(BF)
        return carry

    lax.fori_loop(1, 8, early, 0)

    def recv_2(k, carry):
        i = lax.rem(s + NT - k, NT)
        pltpu.make_async_remote_copy(
            snd2.at[0, 0], got2.at[slot_of(chunk_of(i))], s2.at[k], r2.at[k], device_id={"space": i}
        ).wait_recv()
        return carry

    lax.fori_loop(1, NT, recv_2, 0)
    for place, c in ((9, 0), (0, 7), (19, 8), (10, 15)):

        @pl.when(mine != c)
        def _():
            pltpu.make_async_remote_copy(
                snd2.at[1, 0], got2.at[place], sc.at[0], rc.at[place],
                device_id={"space": device_of(c)},
            ).wait_recv()

    t_got = [
        to_next(2, got2.at[0:20], pgot.at[0:20]),
        to_next(3, got2.at[24:28], pgot.at[20:24]),
        to_next(4, got2.at[32:36], pgot.at[24:28]),
    ]

    @pl.when(sends)
    def _():
        for copy in t_got:
            copy.start()

    r8 = rows((8, L))
    upper = r8 < 4

    def keep(v):
        return jnp.where(later, v, 0.0)

    def wide(ref, i):
        return ref[i].astype(F32)

    def side_pair(m, f, pieces):
        a = jnp.concatenate(pieces, axis=0)
        act[1, m, f] = a.astype(BF)
        act[0, m, f] = down(a, zero_row).astype(BF)
        act[2, m, f] = up(a, zero_row).astype(BF)

    def side_pairs(ref, bases, first, count, into, clean):
        for m, base in zip((0, 9), bases):
            mixed = jnp.zeros((8, L), F32)
            for f in range(4 - count, 4):
                at = base + 2 * (f - 4 + count)
                pieces = [clean(wide(ref, at)), clean(wide(ref, at + 1))]
                side_pair(m, first + f - 4 + count, pieces)
                mixed = jnp.where(r8 == f, pieces[0][0:1], mixed)
                mixed = jnp.where(r8 == 4 + f, pieces[1][7:8], mixed)
            into[m] = mixed

    side_pairs(got2, (28, 20), 2, 4, inner, lambda v: v)
    for m in range(8):
        inner[m + 1] = jnp.where(upper, wide(snd, m), wide(snd, 8 + m))

    def two_frames(half, p, own, prev):
        if half == 1:
            return pltpu.roll(own, 8 - p, 0) if p else own
        if p == 2:
            return own
        if p == 0:
            return pltpu.roll(prev, 6, 0)
        return jnp.where(lax.rem(r8, 4) == 0, pltpu.roll(prev, 5, 0), pltpu.roll(own, 1, 0))

    duo = lax.div(r8, 2)
    none = jnp.zeros((8, L), F32)

    def ring_tiles(half, m):
        own = [wide(got2, 10 + m), wide(got2, m), inner[m]]
        prev = own
        if half == 0:
            prev = [keep(wide(pgot, 10 + m)), keep(wide(pgot, m)), pinner[m]]
        tiles = {}
        for p in range(3):
            t0, b0, o0 = [two_frames(half, p, a, b) for a, b in zip(own, prev)]
            b6 = pltpu.roll(b0, 6, 0)
            low = jnp.where(duo == 1, pltpu.roll(o0, 6, 0), jnp.where(duo == 3, none, t0))
            mid = jnp.where(duo == 0, pltpu.roll(t0, 4, 0), jnp.where(duo == 1, pltpu.roll(b0, 2, 0), none))
            top = jnp.where(duo == 0, o0, jnp.where(duo == 2, none, b6))
            for q, tile in enumerate((low, mid, top)):
                tiles[3 * p + q] = tile.astype(BF)
        return tiles

    for i in range(9):
        ring[1, i, 5, 8:16] = none.astype(BF)

    def rim(half):
        def pairs(u, carry):
            even, odd = ring_tiles(half, 2 * u), ring_tiles(half, 2 * u + 1)
            for i in range(9):
                ring[0, i, u + 1, 0:8] = even[i]
                ring[0, i, u + 1, 8:16] = odd[i]
                ring[1, i, u, 8:16] = even[i]
                ring[1, i, u + 1, 0:8] = odd[i]
            return carry

        lax.fori_loop(0, 5, pairs, 0)
        windows = []
        for p in range(3):
            for q in range(3):
                f = 2 * half + p
                sides = []
                for d in range(2):
                    sides.append(
                        jnp.concatenate(
                            [
                                act[q, d, f : f + 2].reshape(-1, L),
                                act[q, 8 + d, f : f + 2].reshape(-1, L),
                                ring[d, 3 * p + q, 1:6].reshape(-1, L),
                            ],
                            axis=0,
                        )
                    )
                windows.append(jnp.concatenate(sides, axis=1))
        total = conv_rows(windows, near1, far1)
        acc[0, 2 * half : 2 * half + 2] = total[0:32].reshape(2, 16, L)
        acc[8, 2 * half : 2 * half + 2] = total[32:64].reshape(2, 16, L)
        racc[...] = total[64:].reshape(10, 8, L)
        finish(half, 0, 0)
        finish(half, 8, 0)
        lax.fori_loop(1, 8, functools.partial(finish_rows, half), 0)

    def finish(half, m, carry):
        rim_rows = racc[m]
        left_half = lanes((8, L)) < C

        def by_pair(left, middle, right):
            return jnp.where(m == 0, left, middle), jnp.where(m == 8, right, middle)

        t0, t1 = by_pair(near[0], near[1], near[2])
        u0, u1 = by_pair(near[5], near[6], near[7])
        o0, o1 = by_pair(near[3], own_valid, near[4])
        limit = jnp.where(r8 < 2, jnp.where(left_half, t0, t1), jnp.where(left_half, u0, u1))
        outer = norm_silu(rim_rows + bias1, gain2)
        outer = jnp.where(first_frame + 2 * half + lax.rem(r8, 2) < limit, outer, 0.0)
        if half == 1:
            hring[m] = outer.astype(BF)
        limit = jnp.where(lanes((16, L)) < C, o0, o1)
        r16 = rows((16, L))
        for g in range(2):
            f = 2 * half + g
            v = acc[m, f]
            v = v + jnp.where(r16 == 0, rim_rows[4 + g : 5 + g], 0.0)
            v = v + jnp.where(r16 == 15, rim_rows[6 + g : 7 + g], 0.0)
            h = norm_silu(v + bias1, gain2)
            h = jnp.where(first_frame + f < limit, h, 0.0)
            hid[1, m, f + 2] = h.astype(BF)
            hid[0, m, f + 2] = down(h, outer[g : g + 1]).astype(BF)
            hid[2, m, f + 2] = up(h, outer[2 + g : 3 + g]).astype(BF)
        return carry

    def finish_rows(half, m, carry):
        edge = racc[m]
        for g in range(2):
            v = acc[m, 2 * half + g]
            edge = edge + jnp.where(r8 == 4 + g, v[0:1], 0.0) + jnp.where(r8 == 6 + g, v[15:16], 0.0)
        limit = jnp.where(r8 < 2, near[1], jnp.where(r8 < 4, near[6], own_valid))
        edge = norm_silu(edge + bias1, gain2)
        edge = jnp.where(first_frame + 2 * half + lax.rem(r8, 2) < limit, edge, 0.0)
        if half == 1:
            hring[m] = edge.astype(BF)
        r16 = rows((16, L))
        for g in range(2):
            f = 2 * half + g + 2
            above, below = edge[g : g + 1], edge[2 + g : 3 + g]
            first, last = edge[4 + g : 5 + g], edge[6 + g : 7 + g]
            h = hid[1, m, f].astype(F32)
            hid[1, m, f] = jnp.where(r16 == 0, first, jnp.where(r16 == 15, last, h)).astype(BF)
            h = hid[0, m, f].astype(F32)
            hid[0, m, f] = jnp.where(r16 == 0, above, jnp.where(r16 == 1, first, h)).astype(BF)
            h = hid[2, m, f].astype(F32)
            hid[2, m, f] = jnp.where(r16 == 15, below, jnp.where(r16 == 14, last, h)).astype(BF)
        return carry

    rim(1)
    t_hid = [to_next(5, hid.at[1, :, 4:6], phid), to_next(6, hring, phring)]

    @pl.when(sends)
    def _():
        for copy in t_hid:
            copy.start()

    @pl.when(later)
    def _():
        t_snd.wait_recv()
        for copy in t_got:
            copy.wait_recv()

    side_pairs(pgot, (24, 20), 0, 2, pinner, keep)
    for m in range(8):
        pinner[m + 1] = keep(jnp.where(upper, wide(psnd, m), wide(psnd, 8 + m)))
    rim(0)

    def conv2(half):
        windows = []
        for p in range(3):
            for q in range(3):
                f = 2 * half + p
                windows.append(
                    jnp.concatenate(
                        [hid[q, 0:8, f : f + 2].reshape(-1, L), hid[q, 1:9, f : f + 2].reshape(-1, L)],
                        axis=1,
                    )
                )
        total = conv_rows(windows, near2, far2)
        total = total.reshape(8, 2, 16, L)
        for g in range(2):
            f = 2 * half + g
            there = first_frame + f < own_valid
            for m in range(8):
                x = vid[f, :, L * m : L * m + L].astype(F32)
                o = jnp.where(there, total[m, g] + bias2 + x, 0.0)
                out[f, 0, :, L * m : L * m + L] = o.astype(BF)

    conv2(1)

    @pl.when(later)
    def _():
        for copy in t_hid:
            copy.wait_recv()

    def before_2(m, carry):
        rim_rows = keep(phring[m].astype(F32))
        for f in range(2):
            h = keep(phid[m, f].astype(F32))
            hid[1, m, f] = h.astype(BF)
            hid[0, m, f] = down(h, rim_rows[f : f + 1]).astype(BF)
            hid[2, m, f] = up(h, rim_rows[2 + f : 3 + f]).astype(BF)
        return carry

    lax.fori_loop(0, 9, before_2, 0)
    conv2(0)

    def sent(k, carry):
        send_1(k).wait_send()
        send_2(k).wait_send()
        return carry

    lax.fori_loop(1, NT, sent, 0)

    @pl.when(is_corner)
    def _():
        def sent_c(k, carry):
            send_c(k).wait_send()
            return carry

        lax.fori_loop(1, NT, sent_c, 0)

    @pl.when(sends)
    def _():
        for copy in [t_act, t_snd, *t_got, *t_hid]:
            copy.wait_send()


def on_device(video, nbr, vf, g1, w1, b1, g2, w2, b2):
    vmem = lambda *shape, dtype=BF: pltpu.VMEM(shape, dtype)
    dma = lambda n: pltpu.SemaphoreType.DMA((n,))
    hbm = pl.BlockSpec(memory_space=pltpu.HBM)
    local = pl.BlockSpec(memory_space=pltpu.VMEM)
    return pl.pallas_call(
        kernel,
        out_shape=pltpu.VMEM(video.shape, BF),
        in_specs=[hbm] * 9,
        out_specs=local,
        scratch_shapes=[
            pltpu.SMEM((8, NT), jnp.int32),
            pltpu.SMEM((NT,), jnp.int32),
            *[vmem(C, dtype=F32)] * 4,
            vmem(4, 16, 16 * C),
            vmem(9, C, 3 * C),
            vmem(9, C, 3 * C),
            *[vmem(9, C + L + 64, 256)] * 4,
            vmem(3, 10, 6, 16, L),
            vmem(16, 8, L, dtype=F32),
            vmem(32, 8, L),
            vmem(NT + 1, 8, L),
            vmem(2, NT, 8, L),
            vmem(36, 8, L),
            vmem(8, 2, 16, L),
            vmem(16, 8, L),
            vmem(28, 8, L),
            vmem(10, 8, L, dtype=F32),
            vmem(10, 8, L, dtype=F32),
            vmem(2, 9, 6, 16, L),
            vmem(9, 4, 16, L, dtype=F32),
            vmem(10, 8, L, dtype=F32),
            vmem(3, 9, 6, 16, L),
            vmem(9, 8, L),
            vmem(9, 2, 16, L),
            vmem(9, 8, L),
            dma(9), dma(NT), dma(NT), dma(NT), dma(NT), dma(NT), dma(20), dma(7), dma(7),
        ],
        compiler_params=pltpu.CompilerParams(
            collective_id=0, has_side_effects=True, vmem_limit_bytes=66000000
        ),
    )(video, nbr.T, vf, g1, jnp.swapaxes(w1, 1, 2), b1, g2, jnp.swapaxes(w2, 1, 2), b2)


def solution(mesh):
    placed = (P("tm", "space", None, None), P(), P(), P(), P(), P(), P(), P(), P())
    return jax.shard_map(
        on_device, mesh=mesh, in_specs=placed, out_specs=P("tm", "space", None, None), check_vma=False
    )
```
